32 devices in a mesh: energy: 16 (over z, y, core), cuts: 2 (over x).
Axes of the slice: x: 2, y: 2, z: 4, core: 2. Of those that a mesh axis runs over, the one named last changes fastest.
Arguments:
- green: bfloat16 [64, 2, 4, 128, 128], P('energy', 'cuts'), may hold values from -6 to 6
- offsets: int32 [4], replicated, may hold values from 1 to 2
- occupation: float32 [4], replicated, may hold values from 0.05 to 2
- coupling: bfloat16 [4, 3, 2, 128, 128], P(None, None, 'cuts'), may hold values from -0.25 to 0.25
Outputs:
- sigma: float32 [64, 2, 4, 128, 128], P('energy', 'cuts')
The draws below stay inside these ranges and needn't reach their ends.
All inputs are finite; a program needn't handle non-finite values.
Results may differ from the reference program's by a relative error of at most 0.0041.
Values may be sent and summed in bfloat16 or wider, within the bound.
A program may use at most 64 MiB of HBM per device.

```python
import math
import jax
import jax.numpy as jnp
from jax import lax

NO = 128
BR = 4
E_DEV = 4
OFFMAX = 2
NE = 64
NS = 2


def set_ends(values, own_key, low, top_value):
    shape = values.shape
    spot = [jax.random.randint(jax.random.fold_in(own_key, axis), (), 0, shape[axis]) for axis in range(len(shape))]
    values = values.at[tuple(spot)].set(low)
    longest = shape.index(max(shape))
    spot[longest] = (spot[longest] + 1) % shape[longest]
    return values.at[tuple(spot)].set(top_value)


def block_levels(stream_key, dims, cuts, least, largest):
    gain, own = 1.0, jax.random.fold_in(stream_key, 6)
    for dim, shards_of in cuts:
        steps = jnp.exp(jax.random.uniform(jax.random.fold_in(own, dim), (shards_of,), jnp.float32, least / len(cuts), largest / len(cuts)))
        gain = gain * jnp.repeat(steps, dims[dim] // shards_of).reshape([-1 if axis == dim else 1 for axis in range(len(dims))])
    return gain


def centred(own_key, shape, scale, most, pieces=(), kind=jnp.bfloat16):
    loudness = block_levels(own_key, shape, pieces, -0.22, 0.18) if pieces else 1.0
    entries = jax.random.normal(own_key, shape, jnp.float32) * scale * loudness
    return jnp.minimum(jnp.maximum(entries, -most), most).astype(kind)


def setup_inputs(seed: int = 0) -> dict:
    key_list = jax.random.split(jax.random.key(seed), 5)
    return {
        "green": centred(key_list[0], (NE, NS, 4, NO, NO), 1.0, 6.0, ((0, 16), (1, 2))),
        "offsets": set_ends(jax.random.randint(key_list[1], (BR,), 1, OFFMAX + 1), jax.random.fold_in(key_list[1], 1), 1, OFFMAX).astype(jnp.int32),
        "occupation": jnp.clip(jnp.exp(jax.random.uniform(key_list[2], (BR,), jnp.float32, math.log(0.05), math.log(2.0))), 0.05, 2.0),
        "coupling": centred(key_list[3], (BR, 3, NS, NO, NO), (4 * NO) ** -0.5, 0.25, ((2, 2),)),
    }


def self_energy(extended, offsets, occupation, coupling, energies, reach):
    slices = extended.shape[1] - 2
    orbitals = extended.shape[3]
    total = jnp.zeros((energies, slices, 4, orbitals, orbitals), jnp.float32)
    for branch in range(coupling.shape[0]):
        occupied = occupation[branch]
        lower = jnp.stack([occupied, occupied, occupied + 1.0, occupied + 1.0]).reshape(1, 1, 4, 1, 1)
        upper = jnp.stack([occupied + 1.0, occupied + 1.0, occupied, occupied]).reshape(1, 1, 4, 1, 1)
        below = lax.dynamic_slice_in_dim(extended, (reach - offsets[branch]).astype(jnp.int32), energies, 0)
        above = lax.dynamic_slice_in_dim(extended, (reach + offsets[branch]).astype(jnp.int32), energies, 0)
        mixed = (lower * below.astype(jnp.float32) + upper * above.astype(jnp.float32)).astype(jnp.bfloat16)
        for side in range(3):
            part = mixed[:, side:side + slices].astype(jnp.float32)
            block = coupling[branch, side].astype(jnp.float32)
            left = jnp.einsum("sab,escbd->escad", block, part, precision=lax.Precision.HIGHEST).astype(jnp.bfloat16)
            total = total + jnp.einsum("escad,sfd->escaf", left.astype(jnp.float32), block, precision=lax.Precision.HIGHEST)
    return total


def reference(green, offsets, occupation, coupling):
    padded = jnp.pad(green, ((OFFMAX, OFFMAX), (1, 1), (0, 0), (0, 0), (0, 0)))
    starts = jnp.arange(NE // E_DEV, dtype=jnp.int32) * E_DEV

    def one_block(start):
        window = lax.dynamic_slice_in_dim(padded, start.astype(jnp.int32), E_DEV + 2 * OFFMAX, 0)
        return self_energy(window, offsets, occupation, coupling, E_DEV, OFFMAX)

    blocks = lax.map(one_block, starts)
    return blocks.reshape(NE, NS, 4, NO, NO)
```

```python
import functools
import jax
import jax.numpy as jnp
from jax import lax
from jax.experimental import pallas as pl
from jax.experimental.pallas import tpu as pltpu
from jax.sharding import PartitionSpec as P

OFFMAX = 2
MESH = pl.DeviceIdType.MESH


def kernel(n_energy, n_cuts, slots, offsets_in, occupation_in, green, coupling, acc,
           offsets, occupation, ext, kbuf, kt, small_sem, local_sem, k_sem,
           own_send, own_recv, x_send, x_recv, relay_send, relay_recv):
    rank = lax.axis_index("energy")
    cut = lax.axis_index("cuts")
    count, parts = ext.shape[2] - 2 * OFFMAX, ext.shape[1]
    branches, width = kbuf.shape[0], kbuf.shape[2]
    reach = OFFMAX
    first = rank % 2
    second = 1 - first

    def at(energy, slice_):
        return {"energy": energy, "cuts": slice_}

    has = (rank > 0, rank < n_energy - 1)
    beside = (jnp.maximum(rank - 1, 0), jnp.minimum(rank + 1, n_energy - 1))
    if slots == 1:
        partners = [(1, 1, 1 - cut, None, 2 - 2 * cut)]
    elif slots == 2:
        partners = [
            (1, 2, jnp.maximum(cut - 1, 0), cut > 0, 0),
            (2, 1, jnp.minimum(cut + 1, n_cuts - 1), cut < n_cuts - 1, 2),
        ]
    else:
        partners = []

    def when(cond, do):
        if cond is None:
            do()
        else:
            pl.when(cond)(do)

    def exists(p):
        return jnp.where(p == 0, rank, n_energy - 1 - rank) > 0

    def toward(p):
        return jnp.clip(rank + 2 * p - 1, 0, n_energy - 1)

    def source(p):
        return (count - reach) * p + reach

    def landing(p):
        return (count + reach) * (1 - p)

    def edge(p, c):
        return green.at[pl.ds((count - reach) * p, reach), 0, c]

    def own_copy(p, c):
        return pltpu.make_async_remote_copy(
            src_ref=edge(p, c),
            dst_ref=ext.at[0, c, pl.ds(landing(p), reach)],
            send_sem=own_send.at[p, c], recv_sem=own_recv.at[p, c],
            device_id=at(toward(p), cut), device_id_type=MESH)

    def relay_copy(slot, p, c):
        return pltpu.make_async_remote_copy(
            src_ref=ext.at[slot, c, pl.ds(source(p), reach)],
            dst_ref=ext.at[slot, c, pl.ds(landing(p), reach)],
            send_sem=relay_send.at[slot - 1, p, c], recv_sem=relay_recv.at[slot - 1, p, c],
            device_id=at(toward(p), cut), device_id_type=MESH)

    def x_copy(there, partner, p, c):
        return pltpu.make_async_remote_copy(
            src_ref=edge(p, c),
            dst_ref=ext.at[there, c, pl.ds(source(p), reach)],
            send_sem=x_send.at[there - 1, p, c], recv_sem=x_recv.at[there - 1, p, c],
            device_id=at(rank, partner), device_id_type=MESH)

    barrier = pltpu.get_barrier_semaphore()
    for p in range(2):
        pl.when(has[p])(functools.partial(
            pl.semaphore_signal, barrier, inc=1, device_id=at(beside[p], cut), device_id_type=MESH))
    for here, there, partner, cond, side in partners:
        when(cond, functools.partial(
            pl.semaphore_signal, barrier, inc=1, device_id=at(rank, partner), device_id_type=MESH))

    local = [pltpu.make_async_copy(green.at[:, 0, c], ext.at[0, c, pl.ds(reach, count)], local_sem.at[c])
             for c in range(parts)]
    for c in range(parts):
        local[c].start()
    k_copy = pltpu.make_async_copy(coupling.at[:, :, 0], kbuf, k_sem)
    k_copy.start()
    small = [pltpu.make_async_copy(offsets_in, offsets, small_sem.at[0]),
             pltpu.make_async_copy(occupation_in, occupation, small_sem.at[1])]
    for copy in small:
        copy.start()

    peers = sum(flag.astype(jnp.int32) for flag in has)
    for here, there, partner, cond, side in partners:
        peers = peers + (1 if cond is None else cond.astype(jnp.int32))
    pl.semaphore_wait(barrier, peers)

    order = [(0, 0)]
    for c in range(1, parts):
        order += [(0, c), (1, c - 1)]
    order += [(1, parts - 1)]
    for which, c in order:
        p = (first, second)[which]
        for here, there, partner, cond, side in partners:
            when(cond, lambda: x_copy(there, partner, p, c).start())
        if which == 0:
            for q in (first, second):
                pl.when(exists(q))(lambda: own_copy(q, c).start())

    @pl.when(rank == 0)
    def _():
        ext[:, :, pl.ds(0, reach)] = jnp.zeros((slots + 1, parts, reach, width, width), ext.dtype)

    @pl.when(rank == n_energy - 1)
    def _():
        ext[:, :, pl.ds(count + reach, reach)] = jnp.zeros((slots + 1, parts, reach, width, width), ext.dtype)

    k_copy.wait()
    for copy in small + local:
        copy.wait()
    for s in range(kbuf.shape[1]):
        for b in range(branches):
            kt[s, b * width:(b + 1) * width, :] = kbuf[b, s].T

    def forward(which, c):
        p = (first, second)[which]
        for here, there, partner, cond, side in partners:
            def go():
                x_copy(here, partner, p, c).wait_recv()
                pl.when(exists(p))(lambda: relay_copy(here, p, c).start())
            when(cond, go)

    def own_ready(c):
        for p in range(2):
            pl.when(has[p])(lambda: own_copy(1 - p, c).wait_recv())

    steps = parts * (slots + 1)
    last = 2 * parts - 2
    plan = {}
    for position, item in enumerate(order if partners else []):
        plan.setdefault(min(position, last), []).append(item)

    def compute(slot, side, c):
        values = [ext[slot, c, e].astype(jnp.float32) for e in range(count + 2 * reach)]
        lefts = []
        for b in range(branches):
            n = occupation[b]
            w = offsets[b]
            lesser = c < parts // 2
            lower = jnp.where(lesser, n, n + 1.0)
            upper = jnp.where(lesser, n + 1.0, n)
            low = [jnp.where(w == d, lower, 0.0) for d in range(1, reach + 1)]
            up = [jnp.where(w == d, upper, 0.0) for d in range(1, reach + 1)]
            mixed = []
            for e in range(count):
                total = None
                for d in range(1, reach + 1):
                    term = low[d - 1] * values[reach + e - d] + up[d - 1] * values[reach + e + d]
                    total = term if total is None else total + term
                mixed.append(total.astype(jnp.bfloat16))
            lefts.append(jnp.dot(kbuf[b, side], jnp.concatenate(mixed, axis=1),
                                 preferred_element_type=jnp.float32).astype(jnp.bfloat16))
        rows = [jnp.concatenate([left[:, e * width:(e + 1) * width] for left in lefts], axis=1)
                for e in range(count)]
        return jnp.dot(jnp.concatenate(rows, axis=0), kt[side], preferred_element_type=jnp.float32)

    def step(t, carry):
        slot = t // parts
        c = t % parts
        for k, todo in plan.items():
            @pl.when(t == k)
            def _():
                for which, part in todo:
                    forward(which, part)

        @pl.when(slot == 0)
        def _():
            own_ready(c)

        runs = slot == 0
        side = jnp.where(slot == 0, 1, 0)
        for here, there, partner, cond, which_side in partners:
            side = jnp.where(slot == here, which_side, side)
            mine = slot == here
            if cond is not None:
                mine = jnp.logical_and(mine, cond)
            runs = jnp.logical_or(runs, mine)

            @pl.when(mine)
            def _():
                for p in range(2):
                    pl.when(has[p])(lambda: relay_copy(here, 1 - p, c).wait_recv())

        def work():
            sums = compute(slot, side, c)

            @pl.when(slot == 0)
            def _():
                for e in range(count):
                    acc[c, e] = sums[e * width:(e + 1) * width]

            @pl.when(slot > 0)
            def _():
                for e in range(count):
                    acc[c, e] += sums[e * width:(e + 1) * width]

        if slots == 2:
            pl.when(runs)(work)
        else:
            work()

        return carry

    lax.fori_loop(0, steps, step, 0)

    for c in range(parts):
        for p in range(2):
            pl.when(has[p])(lambda: own_copy(p, c).wait_send())
            for here, there, partner, cond, side in partners:
                when(cond, lambda: x_copy(there, partner, p, c).wait_send())
                both = has[p] if cond is None else jnp.logical_and(cond, has[p])
                pl.when(both)(lambda: relay_copy(here, p, c).wait_send())


def write_out(sums, out, sem):
    copies = [pltpu.make_async_copy(sums.at[c], out.at[:, 0, c], sem.at[c]) for c in range(sums.shape[0])]
    for copy in copies:
        copy.start()
    for copy in copies:
        copy.wait()


def body(n_energy, n_cuts, green, offsets, occupation, coupling):
    count, slices, parts, width, _ = green.shape
    branches, sides = coupling.shape[:2]
    assert slices == 1 and count == 2 * OFFMAX
    slots = min(n_cuts - 1, 2)
    sems = max(slots, 1)
    dma = pltpu.SemaphoreType.DMA
    sums = pl.pallas_call(
        functools.partial(kernel, n_energy, n_cuts, slots),
        out_shape=pltpu.VMEM((parts, count, width, width), jnp.float32),
        in_specs=[
            pl.BlockSpec(memory_space=pl.ANY),
            pl.BlockSpec(memory_space=pl.ANY),
            pl.BlockSpec(memory_space=pl.ANY),
            pl.BlockSpec(memory_space=pl.ANY),
        ],
        out_specs=pl.BlockSpec(memory_space=pltpu.VMEM),
        scratch_shapes=[
            pltpu.SMEM(offsets.shape, offsets.dtype),
            pltpu.SMEM(occupation.shape, occupation.dtype),
            pltpu.VMEM((slots + 1, parts, count + 2 * OFFMAX, width, width), jnp.bfloat16),
            pltpu.VMEM((branches, sides, width, width), jnp.bfloat16),
            pltpu.VMEM((sides, branches * width, width), jnp.bfloat16),
            dma((2,)),
            dma((parts,)),
            dma,
            dma((2, parts)),
            dma((2, parts)),
            dma((sems, 2, parts)),
            dma((sems, 2, parts)),
            dma((sems, 2, parts)),
            dma((sems, 2, parts)),
        ],
        compiler_params=pltpu.CompilerParams(collective_id=0, has_side_effects=True),
    )(offsets, occupation, green, coupling)
    return pl.pallas_call(
        write_out,
        out_shape=jax.ShapeDtypeStruct(green.shape, jnp.float32),
        in_specs=[pl.BlockSpec(memory_space=pltpu.VMEM)],
        out_specs=pl.BlockSpec(memory_space=pl.ANY),
        scratch_shapes=[dma((parts,))],
    )(pltpu.with_memory_space_constraint(sums, pltpu.VMEM))


def solution(mesh):
    sizes = dict(mesh.shape)
    in_specs = (P("energy", "cuts", None, None, None), P(), P(), P(None, None, "cuts", None, None))
    out_specs = P("energy", "cuts", None, None, None)
    return jax.shard_map(
        functools.partial(body, sizes["energy"], sizes["cuts"]),
        mesh=mesh, in_specs=in_specs, out_specs=out_specs, check_vma=False)
```

```python
import functools
import jax
import jax.numpy as jnp
from jax import lax
from jax.experimental import pallas as pl
from jax.experimental.pallas import tpu as pltpu
from jax.sharding import PartitionSpec as P

OFFMAX = 2
MESH = pl.DeviceIdType.MESH


def kernel(n_energy, n_cuts, slots, offsets_in, occupation_in, green, coupling, acc,
           offsets, occupation, ext, kbuf, kt, small_sem, local_sem, k_sem,
           own_send, own_recv, x_send, x_recv, relay_send, relay_recv):
    rank = lax.axis_index("energy")
    cut = lax.axis_index("cuts")
    count, parts = ext.shape[2] - 2 * OFFMAX, ext.shape[1]
    branches, width = kbuf.shape[0], kbuf.shape[2]
    reach = OFFMAX
    first = rank % 2
    second = 1 - first

    def at(energy, slice_):
        return {"energy": energy, "cuts": slice_}

    has = (rank > 0, rank < n_energy - 1)
    beside = (jnp.maximum(rank - 1, 0), jnp.minimum(rank + 1, n_energy - 1))
    if slots == 1:
        partners = [(1, 1, 1 - cut, None, 2 - 2 * cut)]
    elif slots == 2:
        partners = [
            (1, 2, jnp.maximum(cut - 1, 0), cut > 0, 0),
            (2, 1, jnp.minimum(cut + 1, n_cuts - 1), cut < n_cuts - 1, 2),
        ]
    else:
        partners = []

    def when(cond, do):
        if cond is None:
            do()
        else:
            pl.when(cond)(do)

    def exists(p):
        return jnp.where(p == 0, rank, n_energy - 1 - rank) > 0

    def toward(p):
        return jnp.clip(rank + 2 * p - 1, 0, n_energy - 1)

    def source(p):
        return (count - reach) * p + reach

    def landing(p):
        return (count + reach) * (1 - p)

    def edge(p, c):
        return green.at[pl.ds((count - reach) * p, reach), 0, c]

    def own_copy(p, c):
        return pltpu.make_async_remote_copy(
            src_ref=edge(p, c),
            dst_ref=ext.at[0, c, pl.ds(landing(p), reach)],
            send_sem=own_send.at[p, c], recv_sem=own_recv.at[p, c],
            device_id=at(toward(p), cut), device_id_type=MESH)

    def relay_copy(slot, p, c):
        return pltpu.make_async_remote_copy(
            src_ref=ext.at[slot, c, pl.ds(source(p), reach)],
            dst_ref=ext.at[slot, c, pl.ds(landing(p), reach)],
            send_sem=relay_send.at[slot - 1, p, c], recv_sem=relay_recv.at[slot - 1, p, c],
            device_id=at(toward(p), cut), device_id_type=MESH)

    def x_copy(there, partner, p, c):
        return pltpu.make_async_remote_copy(
            src_ref=edge(p, c),
            dst_ref=ext.at[there, c, pl.ds(source(p), reach)],
            send_sem=x_send.at[there - 1, p, c], recv_sem=x_recv.at[there - 1, p, c],
            device_id=at(rank, partner), device_id_type=MESH)

    barrier = pltpu.get_barrier_semaphore()
    for p in range(2):
        pl.when(has[p])(functools.partial(
            pl.semaphore_signal, barrier, inc=1, device_id=at(beside[p], cut), device_id_type=MESH))
    for here, there, partner, cond, side in partners:
        when(cond, functools.partial(
            pl.semaphore_signal, barrier, inc=1, device_id=at(rank, partner), device_id_type=MESH))

    local = [pltpu.make_async_copy(green.at[:, 0, c], ext.at[0, c, pl.ds(reach, count)], local_sem.at[c])
             for c in range(parts)]
    for c in range(parts):
        local[c].start()
    k_copy = pltpu.make_async_copy(coupling.at[:, :, 0], kbuf, k_sem)
    k_copy.start()
    small = [pltpu.make_async_copy(offsets_in, offsets, small_sem.at[0]),
             pltpu.make_async_copy(occupation_in, occupation, small_sem.at[1])]
    for copy in small:
        copy.start()

    peers = sum(flag.astype(jnp.int32) for flag in has)
    for here, there, partner, cond, side in partners:
        peers = peers + (1 if cond is None else cond.astype(jnp.int32))
    pl.semaphore_wait(barrier, peers)

    order = [(0, 0)]
    for c in range(1, parts):
        order += [(0, c), (1, c - 1)]
    order += [(1, parts - 1)]
    for which, c in order:
        p = (first, second)[which]
        for here, there, partner, cond, side in partners:
            when(cond, lambda: x_copy(there, partner, p, c).start())
        if which == 0:
            for q in (first, second):
                pl.when(exists(q))(lambda: own_copy(q, c).start())

    @pl.when(rank == 0)
    def _():
        ext[:, :, pl.ds(0, reach)] = jnp.zeros((slots + 1, parts, reach, width, width), ext.dtype)

    @pl.when(rank == n_energy - 1)
    def _():
        ext[:, :, pl.ds(count + reach, reach)] = jnp.zeros((slots + 1, parts, reach, width, width), ext.dtype)

    k_copy.wait()
    for copy in small + local:
        copy.wait()
    for s in range(kbuf.shape[1]):
        for b in range(branches):
            kt[s, b * width:(b + 1) * width, :] = kbuf[b, s].T

    def forward(which, c):
        p = (first, second)[which]
        for here, there, partner, cond, side in partners:
            def go():
                x_copy(here, partner, p, c).wait_recv()
                pl.when(exists(p))(lambda: relay_copy(here, p, c).start())
            when(cond, go)

    def own_ready(c):
        for p in range(2):
            pl.when(has[p])(lambda: own_copy(1 - p, c).wait_recv())

    steps = parts * (slots + 1)
    last = 2 * parts - 2
    plan = {}
    for position, item in enumerate(order if partners else []):
        plan.setdefault(min(position, last), []).append(item)

    def compute(slot, side, c):
        values = [ext[slot, c, e].astype(jnp.float32) for e in range(count + 2 * reach)]
        lefts = []
        for b in range(branches):
            n = occupation[b]
            w = offsets[b]
            lesser = c < parts // 2
            lower = jnp.where(lesser, n, n + 1.0)
            upper = jnp.where(lesser, n + 1.0, n)
            low = [jnp.where(w == d, lower, 0.0) for d in range(1, reach + 1)]
            up = [jnp.where(w == d, upper, 0.0) for d in range(1, reach + 1)]
            mixed = []
            for e in range(count):
                total = None
                for d in range(1, reach + 1):
                    term = low[d - 1] * values[reach + e - d] + up[d - 1] * values[reach + e + d]
                    total = term if total is None else total + term
                mixed.append(total.astype(jnp.bfloat16))
            lefts.append(jnp.dot(kbuf[b, side], jnp.concatenate(mixed, axis=1),
                                 preferred_element_type=jnp.float32).astype(jnp.bfloat16))
        rows = [jnp.concatenate([left[:, e * width:(e + 1) * width] for left in lefts], axis=1)
                for e in range(count)]
        return jnp.dot(jnp.concatenate(rows, axis=0), kt[side], preferred_element_type=jnp.float32)

    def step(t, carry):
        slot = t // parts
        c = t % parts
        for k, todo in plan.items():
            @pl.when(t == k)
            def _():
                for which, part in todo:
                    forward(which, part)

        @pl.when(slot == 0)
        def _():
            own_ready(c)

        runs = slot == 0
        side = jnp.where(slot == 0, 1, 0)
        for here, there, partner, cond, which_side in partners:
            side = jnp.where(slot == here, which_side, side)
            mine = slot == here
            if cond is not None:
                mine = jnp.logical_and(mine, cond)
            runs = jnp.logical_or(runs, mine)

            @pl.when(mine)
            def _():
                for p in range(2):
                    pl.when(has[p])(lambda: relay_copy(here, 1 - p, c).wait_recv())

        def work():
            sums = compute(slot, side, c)

            @pl.when(slot == 0)
            def _():
                for e in range(count):
                    acc[c, e] = sums[e * width:(e + 1) * width]

            @pl.when(slot > 0)
            def _():
                for e in range(count):
                    acc[c, e] += sums[e * width:(e + 1) * width]

        if slots == 2:
            pl.when(runs)(work)
        else:
            work()

        return carry

    lax.fori_loop(0, steps, step, 0)

    for c in range(parts):
        for p in range(2):
            pl.when(has[p])(lambda: own_copy(p, c).wait_send())
            for here, there, partner, cond, side in partners:
                when(cond, lambda: x_copy(there, partner, p, c).wait_send())
                both = has[p] if cond is None else jnp.logical_and(cond, has[p])
                pl.when(both)(lambda: relay_copy(here, p, c).wait_send())


def write_out(sums, out, sem):
    copies = [pltpu.make_async_copy(sums.at[c], out.at[:, 0, c], sem.at[c]) for c in range(sums.shape[0])]
    for copy in copies:
        copy.start()
    for copy in copies:
        copy.wait()


def body(n_energy, n_cuts, green, offsets, occupation, coupling):
    count, slices, parts, width, _ = green.shape
    branches, sides = coupling.shape[:2]
    assert slices == 1 and count == 2 * OFFMAX
    slots = min(n_cuts - 1, 2)
    sems = max(slots, 1)
    dma = pltpu.SemaphoreType.DMA
    sums = pl.pallas_call(
        functools.partial(kernel, n_energy, n_cuts, slots),
        out_shape=pltpu.VMEM((parts, count, width, width), jnp.float32),
        in_specs=[
            pl.BlockSpec(memory_space=pl.ANY),
            pl.BlockSpec(memory_space=pl.ANY),
            pl.BlockSpec(memory_space=pl.ANY),
            pl.BlockSpec(memory_space=pl.ANY),
        ],
        out_specs=pl.BlockSpec(memory_space=pltpu.VMEM),
        scratch_shapes=[
            pltpu.SMEM(offsets.shape, offsets.dtype),
            pltpu.SMEM(occupation.shape, occupation.dtype),
            pltpu.VMEM((slots + 1, parts, count + 2 * OFFMAX, width, width), jnp.bfloat16),
            pltpu.VMEM((branches, sides, width, width), jnp.bfloat16),
            pltpu.VMEM((sides, branches * width, width), jnp.bfloat16),
            dma((2,)),
            dma((parts,)),
            dma,
            dma((2, parts)),
            dma((2, parts)),
            dma((sems, 2, parts)),
            dma((sems, 2, parts)),
            dma((sems, 2, parts)),
            dma((sems, 2, parts)),
        ],
        compiler_params=pltpu.CompilerParams(collective_id=0, has_side_effects=True),
    )(offsets, occupation, green, coupling)
    return pl.pallas_call(
        write_out,
        out_shape=jax.ShapeDtypeStruct(green.shape, jnp.float32),
        in_specs=[pl.BlockSpec(memory_space=pltpu.VMEM)],
        out_specs=pl.BlockSpec(memory_space=pl.ANY),
        scratch_shapes=[dma((parts,))],
    )(pltpu.with_memory_space_constraint(sums, pltpu.VMEM))


def pair_kernel(n_energy, offsets_in, occupation_in, green, coupling, acc,
                offsets, occupation, ext, kbuf, kt, edge_out, edge_in, local_sem,
                reply_x, reply_e, send, x_recv, own_recv, relay_recv, edge_recv):
    rank = lax.axis_index("energy")
    cut = lax.axis_index("cuts")
    reach = OFFMAX
    count, parts, width = ext.shape[1] - 2 * reach, ext.shape[2], ext.shape[3]
    branches = kbuf.shape[1]
    outer = rank % 2
    inner = 1 - outer
    has_outer = jnp.where(outer == 0, rank, n_energy - 1 - rank) > 0
    early = jnp.where(has_outer, outer, inner)
    late = 1 - early
    core_peer = {"energy": rank + 1 - 2 * outer, "cuts": cut}
    chip_peer = {"energy": jnp.clip(rank - 1 + 2 * outer, 0, n_energy - 1), "cuts": cut}
    slice_peer = {"energy": rank, "cuts": 1 - cut}
    told = (rank + cut) % 2 == 1
    tells = (rank + cut) % 2 == 0

    def own_at(p):
        return pl.ds(reach + (count - reach) * p, reach)

    def halo_at(p):
        return pl.ds((count + reach) * p, reach)

    def edge_at(p):
        return pl.ds((count - reach) * p, reach)

    def x_copy(p, c):
        return pltpu.make_async_remote_copy(
            src_ref=green.at[edge_at(p), 0, c], dst_ref=ext.at[1, own_at(p), c],
            send_sem=send.at[0], recv_sem=x_recv.at[p, c], device_id=slice_peer, device_id_type=MESH)

    def own_copy():
        return pltpu.make_async_remote_copy(
            src_ref=green.at[edge_at(inner), 0], dst_ref=ext.at[0, halo_at(outer)],
            send_sem=send.at[1], recv_sem=own_recv, device_id=core_peer, device_id_type=MESH)

    def relay_copy(c):
        return pltpu.make_async_remote_copy(
            src_ref=ext.at[1, own_at(inner), c], dst_ref=ext.at[1, halo_at(outer), c],
            send_sem=send.at[2], recv_sem=relay_recv.at[c], device_id=core_peer, device_id_type=MESH)

    def edge_copy(c):
        return pltpu.make_async_remote_copy(
            src_ref=edge_out.at[c], dst_ref=edge_in.at[c],
            send_sem=send.at[3], recv_sem=edge_recv.at[c], device_id=chip_peer, device_id_type=MESH)

    def signal(sem, device):
        pl.semaphore_signal(sem, inc=1, device_id=device, device_id_type=MESH)

    barrier = pltpu.get_barrier_semaphore()

    @pl.when(tells)
    def _():
        signal(barrier, slice_peer)

    @pl.when(told)
    def _():
        signal(barrier, core_peer)

    @pl.when(jnp.logical_and(told, has_outer))
    def _():
        signal(barrier, chip_peer)

    @pl.when(told)
    def _():
        pl.semaphore_wait(barrier, 1)
        signal(reply_x, slice_peer)

    @pl.when(tells)
    def _():
        pl.semaphore_wait(reply_x, 1)

    for p in (early, late):
        for c in range(parts):
            x_copy(p, c).start()

    local = [pltpu.make_async_copy(green.at[:, 0], ext.at[0, pl.ds(reach, count)], local_sem.at[0]),
             pltpu.make_async_copy(coupling.at[:, 1, 0], kbuf.at[0], local_sem.at[1]),
             pltpu.make_async_copy(coupling.at[:, 2 - 2 * cut, 0], kbuf.at[1], local_sem.at[2]),
             pltpu.make_async_copy(offsets_in, offsets, local_sem.at[3]),
             pltpu.make_async_copy(occupation_in, occupation, local_sem.at[4])]
    for copy in local:
        copy.start()

    @pl.when(tells)
    def _():
        pl.semaphore_wait(barrier, 1 + has_outer.astype(jnp.int32))
        signal(reply_e.at[0], core_peer)

    @pl.when(jnp.logical_and(tells, has_outer))
    def _():
        signal(reply_e.at[1], chip_peer)

    @pl.when(told)
    def _():
        pl.semaphore_wait(reply_e.at[0], 1)

    own_copy().start()

    ext[:, halo_at(outer)] = jnp.zeros((2, reach, parts, width, width), ext.dtype)
    for copy in local:
        copy.wait()
    for s in range(2):
        for b in range(branches):
            kt[s, b * width:(b + 1) * width, :] = kbuf[s, b].T

    @pl.when(jnp.logical_and(told, has_outer))
    def _():
        pl.semaphore_wait(reply_e.at[1], 1)

    own_copy().wait_recv()

    def weights(c):
        lesser = c < parts // 2
        lower = [jnp.where(lesser, occupation[b], occupation[b] + 1.0) for b in range(branches)]
        upper = [jnp.where(lesser, occupation[b] + 1.0, occupation[b]) for b in range(branches)]
        return lower, upper, [offsets[b] == 1 for b in range(branches)]

    def unit(s, c):
        lower, upper, near = weights(c)
        values = [ext[s, e, c].astype(jnp.float32) for e in range(count + 2 * reach)]
        lefts = []
        for b in range(branches):
            mixed = []
            for e in range(reach, reach + count):
                below = jnp.where(near[b], values[e - 1], values[e - 2])
                above = jnp.where(near[b], values[e + 1], values[e + 2])
                mixed.append((lower[b] * below + upper[b] * above).astype(jnp.bfloat16))
            lefts.append(jnp.dot(kbuf[s, b], jnp.concatenate(mixed, axis=1),
                                 preferred_element_type=jnp.float32).astype(jnp.bfloat16))
        rows = [jnp.concatenate([left[:, e * width:(e + 1) * width] for left in lefts], axis=1)
                for e in range(count)]
        return jnp.dot(jnp.concatenate(rows, axis=0), kt[s], preferred_element_type=jnp.float32)

    def edge(c):
        lower, upper, near = weights(c)
        lefts = []
        for s in range(2):
            first = ext[s, reach + (count - 1) * outer, c].astype(jnp.float32)
            second = ext[s, reach + 1 + (count - 3) * outer, c].astype(jnp.float32)
            for b in range(branches):
                gain = jnp.where(outer == 0, upper[b], lower[b])
                one = gain * jnp.where(near[b], first, second)
                two = jnp.where(near[b], 0.0, gain) * first
                both = jnp.concatenate([one.astype(jnp.bfloat16), two.astype(jnp.bfloat16)], axis=1)
                lefts.append(jnp.dot(kbuf[s, b], both, preferred_element_type=jnp.float32).astype(jnp.bfloat16))
        rows = [jnp.concatenate([left[:, e * width:(e + 1) * width] for left in lefts], axis=1)
                for e in range(reach)]
        sums = jnp.dot(jnp.concatenate(rows, axis=0), kt[...].reshape(2 * branches * width, width),
                       preferred_element_type=jnp.float32).astype(edge_out.dtype)
        for e in range(reach):
            edge_out[c, e] = sums[e * width:(e + 1) * width]

    def first_half(c, carry):
        sums = unit(0, c)
        for e in range(count):
            acc[e, c] = sums[e * width:(e + 1) * width]

        @pl.when(jnp.logical_and(has_outer, c > 0))
        def _():
            edge_copy(c - 1).start()

        x_copy(early, c).wait_recv()

        @pl.when(has_outer)
        def _():
            edge(c)

        @pl.when(jnp.logical_not(has_outer))
        def _():
            relay_copy(c).start()

        return carry

    lax.fori_loop(0, parts, first_half, 0)

    def second_half(t, carry):
        @pl.when(t < parts)
        def _():
            x_copy(late, t).wait_recv()
            pl.when(has_outer)(lambda: relay_copy(t).start())

        @pl.when(jnp.logical_and(has_outer, t == 0))
        def _():
            edge_copy(parts - 1).start()

        @pl.when(t > 0)
        def _():
            c = t - 1
            relay_copy(c).wait_recv()
            sums = unit(1, c)
            for e in range(count):
                acc[e, c] += sums[e * width:(e + 1) * width]

            @pl.when(has_outer)
            def _():
                edge_copy(c).wait_recv()
                acc[(count - 1) * outer, c] += edge_in[c, 0].astype(jnp.float32)
                acc[1 + (count - 3) * outer, c] += edge_in[c, 1].astype(jnp.float32)

        return carry

    lax.fori_loop(0, parts + 1, second_half, 0)

    def sent(ref, n):
        pltpu.make_async_copy(ref, ref, send.at[n]).wait()

    sent(ext.at[1, pl.ds(reach, count)], 0)
    sent(ext.at[0, pl.ds(0, reach)], 1)
    sent(ext.at[1, pl.ds(0, reach)], 2)
    pl.when(has_outer)(lambda: sent(edge_out, 3))


def pair_write(sums, out, sem):
    parts = sums.shape[1]
    copies = [pltpu.make_async_copy(sums.at[:, c], out.at[:, 0, c], sem.at[c]) for c in range(parts)]
    for copy in copies:
        copy.start()
    for copy in copies:
        copy.wait()


def pair_body(n_energy, green, offsets, occupation, coupling):
    count, slices, parts, width, _ = green.shape
    branches = coupling.shape[0]
    assert slices == 1 and count == 2 * OFFMAX
    dma = pltpu.SemaphoreType.DMA
    regular = pltpu.SemaphoreType.REGULAR
    sums = pl.pallas_call(
        functools.partial(pair_kernel, n_energy),
        out_shape=pltpu.VMEM((count, parts, width, width), jnp.float32),
        in_specs=[pl.BlockSpec(memory_space=pl.ANY)] * 4,
        out_specs=pl.BlockSpec(memory_space=pltpu.VMEM),
        scratch_shapes=[
            pltpu.SMEM(offsets.shape, offsets.dtype),
            pltpu.SMEM(occupation.shape, occupation.dtype),
            pltpu.VMEM((2, count + 2 * OFFMAX, parts, width, width), jnp.bfloat16),
            pltpu.VMEM((2, branches, width, width), jnp.bfloat16),
            pltpu.VMEM((2, branches * width, width), jnp.bfloat16),
            pltpu.VMEM((parts, OFFMAX, width, width), jnp.bfloat16),
            pltpu.VMEM((parts, OFFMAX, width, width), jnp.bfloat16),
            dma((5,)),
            regular,
            regular((2,)),
            dma((4,)),
            dma((2, parts)),
            dma,
            dma((parts,)),
            dma((parts,)),
        ],
        compiler_params=pltpu.CompilerParams(collective_id=0, has_side_effects=True),
    )(offsets, occupation, green, coupling)
    return pl.pallas_call(
        pair_write,
        out_shape=jax.ShapeDtypeStruct(green.shape, jnp.float32),
        in_specs=[pl.BlockSpec(memory_space=pltpu.VMEM)],
        out_specs=pl.BlockSpec(memory_space=pl.ANY),
        scratch_shapes=[dma((parts,))],
    )(pltpu.with_memory_space_constraint(sums, pltpu.VMEM))


def solution(mesh):
    sizes = dict(mesh.shape)
    in_specs = (P("energy", "cuts", None, None, None), P(), P(), P(None, None, "cuts", None, None))
    out_specs = P("energy", "cuts", None, None, None)
    if sizes["cuts"] == 2 and sizes["energy"] % 2 == 0:
        step = functools.partial(pair_body, sizes["energy"])
    else:
        step = functools.partial(body, sizes["energy"], sizes["cuts"])
    return jax.shard_map(step, mesh=mesh, in_specs=in_specs, out_specs=out_specs, check_vma=False)
```

```python
import functools
import jax
import jax.numpy as jnp
from jax import lax
from jax.experimental import pallas as pl
from jax.experimental.pallas import tpu as pltpu
from jax.sharding import PartitionSpec as P

OFFMAX = 2
HOLD = ((3, 3, 4, 4), (2, 2, 3, 3))
MESH = pl.DeviceIdType.MESH


def kernel(n_energy, n_cuts, slots, offsets_in, occupation_in, green, coupling, acc,
           offsets, occupation, ext, kbuf, kt, small_sem, local_sem, k_sem,
           own_send, own_recv, x_send, x_recv, relay_send, relay_recv):
    rank = lax.axis_index("energy")
    cut = lax.axis_index("cuts")
    count, parts = ext.shape[2] - 2 * OFFMAX, ext.shape[1]
    branches, width = kbuf.shape[0], kbuf.shape[2]
    reach = OFFMAX
    first = rank % 2
    second = 1 - first

    def at(energy, slice_):
        return {"energy": energy, "cuts": slice_}

    has = (rank > 0, rank < n_energy - 1)
    beside = (jnp.maximum(rank - 1, 0), jnp.minimum(rank + 1, n_energy - 1))
    if slots == 1:
        partners = [(1, 1, 1 - cut, None, 2 - 2 * cut)]
    elif slots == 2:
        partners = [
            (1, 2, jnp.maximum(cut - 1, 0), cut > 0, 0),
            (2, 1, jnp.minimum(cut + 1, n_cuts - 1), cut < n_cuts - 1, 2),
        ]
    else:
        partners = []

    def when(cond, do):
        if cond is None:
            do()
        else:
            pl.when(cond)(do)

    def exists(p):
        return jnp.where(p == 0, rank, n_energy - 1 - rank) > 0

    def toward(p):
        return jnp.clip(rank + 2 * p - 1, 0, n_energy - 1)

    def source(p):
        return (count - reach) * p + reach

    def landing(p):
        return (count + reach) * (1 - p)

    def edge(p, c):
        return green.at[pl.ds((count - reach) * p, reach), 0, c]

    def own_copy(p, c):
        return pltpu.make_async_remote_copy(
            src_ref=edge(p, c),
            dst_ref=ext.at[0, c, pl.ds(landing(p), reach)],
            send_sem=own_send.at[p, c], recv_sem=own_recv.at[p, c],
            device_id=at(toward(p), cut), device_id_type=MESH)

    def relay_copy(slot, p, c):
        return pltpu.make_async_remote_copy(
            src_ref=ext.at[slot, c, pl.ds(source(p), reach)],
            dst_ref=ext.at[slot, c, pl.ds(landing(p), reach)],
            send_sem=relay_send.at[slot - 1, p, c], recv_sem=relay_recv.at[slot - 1, p, c],
            device_id=at(toward(p), cut), device_id_type=MESH)

    def x_copy(there, partner, p, c):
        return pltpu.make_async_remote_copy(
            src_ref=edge(p, c),
            dst_ref=ext.at[there, c, pl.ds(source(p), reach)],
            send_sem=x_send.at[there - 1, p, c], recv_sem=x_recv.at[there - 1, p, c],
            device_id=at(rank, partner), device_id_type=MESH)

    barrier = pltpu.get_barrier_semaphore()
    for p in range(2):
        pl.when(has[p])(functools.partial(
            pl.semaphore_signal, barrier, inc=1, device_id=at(beside[p], cut), device_id_type=MESH))
    for here, there, partner, cond, side in partners:
        when(cond, functools.partial(
            pl.semaphore_signal, barrier, inc=1, device_id=at(rank, partner), device_id_type=MESH))

    local = [pltpu.make_async_copy(green.at[:, 0, c], ext.at[0, c, pl.ds(reach, count)], local_sem.at[c])
             for c in range(parts)]
    for c in range(parts):
        local[c].start()
    k_copy = pltpu.make_async_copy(coupling.at[:, :, 0], kbuf, k_sem)
    k_copy.start()
    small = [pltpu.make_async_copy(offsets_in, offsets, small_sem.at[0]),
             pltpu.make_async_copy(occupation_in, occupation, small_sem.at[1])]
    for copy in small:
        copy.start()

    peers = sum(flag.astype(jnp.int32) for flag in has)
    for here, there, partner, cond, side in partners:
        peers = peers + (1 if cond is None else cond.astype(jnp.int32))
    pl.semaphore_wait(barrier, peers)

    order = [(0, 0)]
    for c in range(1, parts):
        order += [(0, c), (1, c - 1)]
    order += [(1, parts - 1)]
    for which, c in order:
        p = (first, second)[which]
        for here, there, partner, cond, side in partners:
            when(cond, lambda: x_copy(there, partner, p, c).start())
        if which == 0:
            for q in (first, second):
                pl.when(exists(q))(lambda: own_copy(q, c).start())

    @pl.when(rank == 0)
    def _():
        ext[:, :, pl.ds(0, reach)] = jnp.zeros((slots + 1, parts, reach, width, width), ext.dtype)

    @pl.when(rank == n_energy - 1)
    def _():
        ext[:, :, pl.ds(count + reach, reach)] = jnp.zeros((slots + 1, parts, reach, width, width), ext.dtype)

    k_copy.wait()
    for copy in small + local:
        copy.wait()
    for s in range(kbuf.shape[1]):
        for b in range(branches):
            kt[s, b * width:(b + 1) * width, :] = kbuf[b, s].T

    def forward(which, c):
        p = (first, second)[which]
        for here, there, partner, cond, side in partners:
            def go():
                x_copy(here, partner, p, c).wait_recv()
                pl.when(exists(p))(lambda: relay_copy(here, p, c).start())
            when(cond, go)

    def own_ready(c):
        for p in range(2):
            pl.when(has[p])(lambda: own_copy(1 - p, c).wait_recv())

    steps = parts * (slots + 1)
    last = 2 * parts - 2
    plan = {}
    for position, item in enumerate(order if partners else []):
        plan.setdefault(min(position, last), []).append(item)

    def compute(slot, side, c):
        values = [ext[slot, c, e].astype(jnp.float32) for e in range(count + 2 * reach)]
        lefts = []
        for b in range(branches):
            n = occupation[b]
            w = offsets[b]
            lesser = c < parts // 2
            lower = jnp.where(lesser, n, n + 1.0)
            upper = jnp.where(lesser, n + 1.0, n)
            low = [jnp.where(w == d, lower, 0.0) for d in range(1, reach + 1)]
            up = [jnp.where(w == d, upper, 0.0) for d in range(1, reach + 1)]
            mixed = []
            for e in range(count):
                total = None
                for d in range(1, reach + 1):
                    term = low[d - 1] * values[reach + e - d] + up[d - 1] * values[reach + e + d]
                    total = term if total is None else total + term
                mixed.append(total.astype(jnp.bfloat16))
            lefts.append(jnp.dot(kbuf[b, side], jnp.concatenate(mixed, axis=1),
                                 preferred_element_type=jnp.float32).astype(jnp.bfloat16))
        rows = [jnp.concatenate([left[:, e * width:(e + 1) * width] for left in lefts], axis=1)
                for e in range(count)]
        return jnp.dot(jnp.concatenate(rows, axis=0), kt[side], preferred_element_type=jnp.float32)

    def step(t, carry):
        slot = t // parts
        c = t % parts
        for k, todo in plan.items():
            @pl.when(t == k)
            def _():
                for which, part in todo:
                    forward(which, part)

        @pl.when(slot == 0)
        def _():
            own_ready(c)

        runs = slot == 0
        side = jnp.where(slot == 0, 1, 0)
        for here, there, partner, cond, which_side in partners:
            side = jnp.where(slot == here, which_side, side)
            mine = slot == here
            if cond is not None:
                mine = jnp.logical_and(mine, cond)
            runs = jnp.logical_or(runs, mine)

            @pl.when(mine)
            def _():
                for p in range(2):
                    pl.when(has[p])(lambda: relay_copy(here, 1 - p, c).wait_recv())

        def work():
            sums = compute(slot, side, c)

            @pl.when(slot == 0)
            def _():
                for e in range(count):
                    acc[c, e] = sums[e * width:(e + 1) * width]

            @pl.when(slot > 0)
            def _():
                for e in range(count):
                    acc[c, e] += sums[e * width:(e + 1) * width]

        if slots == 2:
            pl.when(runs)(work)
        else:
            work()

        return carry

    lax.fori_loop(0, steps, step, 0)

    for c in range(parts):
        for p in range(2):
            pl.when(has[p])(lambda: own_copy(p, c).wait_send())
            for here, there, partner, cond, side in partners:
                when(cond, lambda: x_copy(there, partner, p, c).wait_send())
                both = has[p] if cond is None else jnp.logical_and(cond, has[p])
                pl.when(both)(lambda: relay_copy(here, p, c).wait_send())


def write_out(sums, out, sem):
    copies = [pltpu.make_async_copy(sums.at[c], out.at[:, 0, c], sem.at[c]) for c in range(sums.shape[0])]
    for copy in copies:
        copy.start()
    for copy in copies:
        copy.wait()


def body(n_energy, n_cuts, green, offsets, occupation, coupling):
    count, slices, parts, width, _ = green.shape
    branches, sides = coupling.shape[:2]
    assert slices == 1 and count == 2 * OFFMAX
    slots = min(n_cuts - 1, 2)
    sems = max(slots, 1)
    dma = pltpu.SemaphoreType.DMA
    sums = pl.pallas_call(
        functools.partial(kernel, n_energy, n_cuts, slots),
        out_shape=pltpu.VMEM((parts, count, width, width), jnp.float32),
        in_specs=[
            pl.BlockSpec(memory_space=pl.ANY),
            pl.BlockSpec(memory_space=pl.ANY),
            pl.BlockSpec(memory_space=pl.ANY),
            pl.BlockSpec(memory_space=pl.ANY),
        ],
        out_specs=pl.BlockSpec(memory_space=pltpu.VMEM),
        scratch_shapes=[
            pltpu.SMEM(offsets.shape, offsets.dtype),
            pltpu.SMEM(occupation.shape, occupation.dtype),
            pltpu.VMEM((slots + 1, parts, count + 2 * OFFMAX, width, width), jnp.bfloat16),
            pltpu.VMEM((branches, sides, width, width), jnp.bfloat16),
            pltpu.VMEM((sides, branches * width, width), jnp.bfloat16),
            dma((2,)),
            dma((parts,)),
            dma,
            dma((2, parts)),
            dma((2, parts)),
            dma((sems, 2, parts)),
            dma((sems, 2, parts)),
            dma((sems, 2, parts)),
            dma((sems, 2, parts)),
        ],
        compiler_params=pltpu.CompilerParams(collective_id=0, has_side_effects=True),
    )(offsets, occupation, green, coupling)
    return pl.pallas_call(
        write_out,
        out_shape=jax.ShapeDtypeStruct(green.shape, jnp.float32),
        in_specs=[pl.BlockSpec(memory_space=pltpu.VMEM)],
        out_specs=pl.BlockSpec(memory_space=pl.ANY),
        scratch_shapes=[dma((parts,))],
    )(pltpu.with_memory_space_constraint(sums, pltpu.VMEM))


def targets(values, k, k_t, lower, upper, near):
    width, reach = k_t.shape[1], OFFMAX
    count = len(values) - 2 * reach
    lefts = []
    for b in range(k.shape[0]):
        mixed = []
        for e in range(reach, reach + count):
            below = jnp.where(near[b], values[e - 1], values[e - 2])
            above = jnp.where(near[b], values[e + 1], values[e + 2])
            mixed.append((lower[b] * below + upper[b] * above).astype(jnp.bfloat16))
        lefts.append(jnp.dot(k[b], jnp.concatenate(mixed, axis=1),
                             preferred_element_type=jnp.float32).astype(jnp.bfloat16))
    return [jnp.dot(jnp.concatenate([left[:, e * width:(e + 1) * width] for left in lefts], axis=1), k_t[...],
                    preferred_element_type=jnp.float32) for e in range(count)]


def pair_kernel(n_energy, offsets_in, occupation_in, green, coupling, acc, far, kbuf, kt, scales,
                offsets, occupation, own, edge_out, edge_in, local_sem,
                reply_x, reply_e, send, x_recv, own_recv, relay_recv, edge_recv):
    rank = lax.axis_index("energy")
    cut = lax.axis_index("cuts")
    reach = OFFMAX
    count, parts, width = own.shape[0] - 2 * reach, own.shape[1], own.shape[2]
    branches = kbuf.shape[1]
    outer = rank % 2
    inner = 1 - outer
    has_outer = jnp.where(outer == 0, rank, n_energy - 1 - rank) > 0
    early = jnp.where(has_outer, outer, inner)
    late = 1 - early
    core_peer = {"energy": rank + 1 - 2 * outer, "cuts": cut}
    chip_peer = {"energy": jnp.clip(rank - 1 + 2 * outer, 0, n_energy - 1), "cuts": cut}
    slice_peer = {"energy": rank, "cuts": 1 - cut}
    told = (rank + cut) % 2 == 0
    tells = (rank + cut) % 2 == 1

    def own_at(p):
        return pl.ds(reach + (count - reach) * p, reach)

    def halo_at(p):
        return pl.ds((count + reach) * p, reach)

    def edge_at(p):
        return pl.ds((count - reach) * p, reach)

    def x_copy(p, c):
        return pltpu.make_async_remote_copy(
            src_ref=green.at[edge_at(p), 0, c], dst_ref=far.at[own_at(p), c],
            send_sem=send.at[0], recv_sem=x_recv.at[p, c], device_id=slice_peer, device_id_type=MESH)

    def own_copy():
        return pltpu.make_async_remote_copy(
            src_ref=green.at[edge_at(inner), 0], dst_ref=own.at[halo_at(outer)],
            send_sem=send.at[1], recv_sem=own_recv, device_id=core_peer, device_id_type=MESH)

    def relay_copy(c):
        return pltpu.make_async_remote_copy(
            src_ref=far.at[own_at(inner), c], dst_ref=far.at[halo_at(outer), c],
            send_sem=send.at[2], recv_sem=relay_recv.at[c], device_id=core_peer, device_id_type=MESH)

    def edge_copy(c):
        return pltpu.make_async_remote_copy(
            src_ref=edge_out.at[c], dst_ref=edge_in.at[c],
            send_sem=send.at[3], recv_sem=edge_recv.at[c], device_id=chip_peer, device_id_type=MESH)

    def signal(sem, device):
        pl.semaphore_signal(sem, inc=1, device_id=device, device_id_type=MESH)

    barrier = pltpu.get_barrier_semaphore()

    @pl.when(tells)
    def _():
        signal(barrier, slice_peer)

    @pl.when(told)
    def _():
        signal(barrier, core_peer)

    @pl.when(jnp.logical_and(told, has_outer))
    def _():
        signal(barrier, chip_peer)

    @pl.when(told)
    def _():
        pl.semaphore_wait(barrier, 1)
        signal(reply_x, slice_peer)

    @pl.when(tells)
    def _():
        pl.semaphore_wait(reply_x, 1)

    held_back = jnp.logical_and(outer == 1, rank > 1)
    longer = jnp.logical_and(cut == 0, has_outer)
    for c in range(parts):
        x_copy(early, c).start()

    @pl.when(jnp.logical_not(held_back))
    def _():
        for c in range(parts):
            x_copy(late, c).start()

    def release(point):
        for c in range(parts):
            at = jnp.where(longer, HOLD[0][c], HOLD[1][c])
            pl.when(jnp.logical_and(held_back, point == at))(lambda: x_copy(late, c).start())

    local = [pltpu.make_async_copy(green.at[:, 0], own.at[pl.ds(reach, count)], local_sem.at[0]),
             pltpu.make_async_copy(coupling.at[:, 1, 0], kbuf.at[0], local_sem.at[1]),
             pltpu.make_async_copy(coupling.at[:, 2 - 2 * cut, 0], kbuf.at[1], local_sem.at[2]),
             pltpu.make_async_copy(offsets_in, offsets, local_sem.at[3]),
             pltpu.make_async_copy(occupation_in, occupation, local_sem.at[4])]
    for copy in local:
        copy.start()

    @pl.when(tells)
    def _():
        pl.semaphore_wait(barrier, 1 + has_outer.astype(jnp.int32))
        signal(reply_e.at[0], core_peer)

    @pl.when(jnp.logical_and(tells, has_outer))
    def _():
        signal(reply_e.at[1], chip_peer)

    @pl.when(told)
    def _():
        pl.semaphore_wait(reply_e.at[0], 1)

    own_copy().start()

    own[halo_at(outer)] = jnp.zeros((reach, parts, width, width), own.dtype)
    far[halo_at(outer)] = jnp.zeros((reach, parts, width, width), far.dtype)
    for copy in local:
        copy.wait()
    for s in range(2):
        for b in range(branches):
            kt[s, b * width:(b + 1) * width, :] = kbuf[s, b].T

    @pl.when(jnp.logical_and(told, has_outer))
    def _():
        pl.semaphore_wait(reply_e.at[1], 1)

    own_copy().wait_recv()

    def weights(c):
        lesser = c < parts // 2
        lower = [jnp.where(lesser, occupation[b], occupation[b] + 1.0) for b in range(branches)]
        upper = [jnp.where(lesser, occupation[b] + 1.0, occupation[b]) for b in range(branches)]
        return lower, upper, [offsets[b] == 1 for b in range(branches)]

    def unit(blocks, s, c):
        values = [blocks[e, c].astype(jnp.float32) for e in range(count + 2 * reach)]
        return targets(values, kbuf.at[s], kt.at[s], *weights(c))

    def edge(c):
        lower, upper, near = weights(c)
        lefts = []
        for s, blocks in enumerate((own, far)):
            first = blocks[reach + (count - 1) * outer, c].astype(jnp.float32)
            second = blocks[reach + 1 + (count - 3) * outer, c].astype(jnp.float32)
            for b in range(branches):
                gain = jnp.where(outer == 0, upper[b], lower[b])
                one = gain * jnp.where(near[b], first, second)
                two = jnp.where(near[b], 0.0, gain) * first
                both = jnp.concatenate([one.astype(jnp.bfloat16), two.astype(jnp.bfloat16)], axis=1)
                lefts.append(jnp.dot(kbuf[s, b], both, preferred_element_type=jnp.float32).astype(jnp.bfloat16))
        rows = [jnp.concatenate([left[:, e * width:(e + 1) * width] for left in lefts], axis=1)
                for e in range(reach)]
        sums = jnp.dot(jnp.concatenate(rows, axis=0), kt[...].reshape(2 * branches * width, width),
                       preferred_element_type=jnp.float32).astype(edge_out.dtype)
        for e in range(reach):
            edge_out[c, e] = sums[e * width:(e + 1) * width]

    def first_half(c, carry):
        x_copy(early, c).wait_recv()
        release(c)

        @pl.when(has_outer)
        def _():
            edge(c)

        @pl.when(jnp.logical_not(has_outer))
        def _():
            relay_copy(c).start()

        sums = unit(own, 0, c)
        for e in range(count):
            acc[e, c] = sums[e]
        pl.when(has_outer)(lambda: edge_copy(c).start())
        return carry

    lax.fori_loop(0, parts, first_half, 0)

    def arrived(c):
        x_copy(late, c).wait_recv()
        release(parts + c)
        pl.when(has_outer)(lambda: relay_copy(c).start())

    def halo(c):
        relay_copy(c).wait_recv()

        @pl.when(has_outer)
        def _():
            edge_copy(c).wait_recv()
            acc[(count - 1) * outer, c] += edge_in[c, 0].astype(jnp.float32)
            acc[1 + (count - 3) * outer, c] += edge_in[c, 1].astype(jnp.float32)

    pl.when(has_outer)(lambda: arrived(0))

    def second_half(c, carry):
        pl.when(has_outer)(lambda: arrived(c + 1))
        pl.when(jnp.logical_not(has_outer))(lambda: arrived(c))
        halo(c)
        sums = unit(far, 1, c)
        for e in range(count):
            acc[e, c] += sums[e]
        return carry

    lax.fori_loop(0, parts - 1, second_half, 0)
    lower, upper, near = weights(parts - 1)
    for b in range(branches):
        for i, value in enumerate((lower[b], upper[b], jnp.where(near[b], 1.0, 0.0))):
            scales[i, pl.ds(b, 1)] = jnp.full((1, width), value, jnp.float32)
    pl.when(jnp.logical_not(has_outer))(lambda: arrived(parts - 1))
    halo(parts - 1)

    def sent(ref, n):
        pltpu.make_async_copy(ref, ref, send.at[n]).wait()

    sent(far.at[pl.ds(reach, count)], 0)
    sent(own.at[pl.ds(0, reach)], 1)
    sent(far.at[pl.ds(0, reach)], 2)
    pl.when(has_outer)(lambda: sent(edge_out, 3))


def pair_finish(sums, far, kbuf, kt, scales, out, held, write, last_write):
    count, parts = sums.shape[:2]
    last = parts - 1
    copies = [pltpu.make_async_copy(sums.at[:, c], out.at[:, 0, c], write.at[c]) for c in range(last)]
    for copy in copies:
        copy.start()
    branches = range(kbuf.shape[1])
    values = [far[e, last].astype(jnp.float32) for e in range(far.shape[0])]
    rows = [[scales[i, pl.ds(b, 1)] for b in branches] for i in range(3)]
    terms = targets(values, kbuf.at[1], kt.at[1], rows[0], rows[1], [row > 0.5 for row in rows[2]])
    for e in range(count):
        held[e] = sums[e, last] + terms[e]
        copies.append(pltpu.make_async_copy(held.at[e], out.at[e, 0, last], last_write.at[e]))
        copies[-1].start()
    for copy in copies:
        copy.wait()


def pair_body(n_energy, green, offsets, occupation, coupling):
    count, slices, parts, width, _ = green.shape
    branches = coupling.shape[0]
    assert slices == 1 and count == 2 * OFFMAX
    dma = pltpu.SemaphoreType.DMA
    regular = pltpu.SemaphoreType.REGULAR
    vmem = pl.BlockSpec(memory_space=pltpu.VMEM)
    made = pl.pallas_call(
        functools.partial(pair_kernel, n_energy),
        out_shape=[
            pltpu.VMEM((count, parts, width, width), jnp.float32),
            pltpu.VMEM((count + 2 * OFFMAX, parts, width, width), jnp.bfloat16),
            pltpu.VMEM((2, branches, width, width), jnp.bfloat16),
            pltpu.VMEM((2, branches * width, width), jnp.bfloat16),
            pltpu.VMEM((3, branches, width), jnp.float32),
        ],
        in_specs=[pl.BlockSpec(memory_space=pl.ANY)] * 4,
        out_specs=[vmem] * 5,
        scratch_shapes=[
            pltpu.SMEM(offsets.shape, offsets.dtype),
            pltpu.SMEM(occupation.shape, occupation.dtype),
            pltpu.VMEM((count + 2 * OFFMAX, parts, width, width), jnp.bfloat16),
            pltpu.VMEM((parts, OFFMAX, width, width), jnp.bfloat16),
            pltpu.VMEM((parts, OFFMAX, width, width), jnp.bfloat16),
            dma((5,)),
            regular,
            regular((2,)),
            dma((4,)),
            dma((2, parts)),
            dma,
            dma((parts,)),
            dma((parts,)),
        ],
        compiler_params=pltpu.CompilerParams(collective_id=0, has_side_effects=True),
    )(offsets, occupation, green, coupling)
    return pl.pallas_call(
        pair_finish,
        out_shape=jax.ShapeDtypeStruct(green.shape, jnp.float32),
        in_specs=[vmem] * 5,
        out_specs=pl.BlockSpec(memory_space=pl.ANY),
        scratch_shapes=[pltpu.VMEM((count, width, width), jnp.float32), dma((parts,)), dma((count,))],
    )(*[pltpu.with_memory_space_constraint(x, pltpu.VMEM) for x in made])


def solution(mesh):
    sizes = dict(mesh.shape)
    in_specs = (P("energy", "cuts", None, None, None), P(), P(), P(None, None, "cuts", None, None))
    out_specs = P("energy", "cuts", None, None, None)
    if sizes["cuts"] == 2 and sizes["energy"] % 2 == 0:
        step = functools.partial(pair_body, sizes["energy"])
    else:
        step = functools.partial(body, sizes["energy"], sizes["cuts"])
    return jax.shard_map(step, mesh=mesh, in_specs=in_specs, out_specs=out_specs, check_vma=False)
```

```python
import functools
import jax
import jax.numpy as jnp
from jax import lax
from jax.experimental import pallas as pl
from jax.experimental.pallas import tpu as pltpu
from jax.sharding import PartitionSpec as P

OFFMAX = 2
HOLD = ((3, 3, 4, 4), (2, 2, 3, 3))
MESH = pl.DeviceIdType.MESH


def kernel(n_energy, n_cuts, slots, offsets_in, occupation_in, green, coupling, acc,
           offsets, occupation, ext, kbuf, kt, small_sem, local_sem, k_sem,
           own_send, own_recv, x_send, x_recv, relay_send, relay_recv):
    rank = lax.axis_index("energy")
    cut = lax.axis_index("cuts")
    count, parts = ext.shape[2] - 2 * OFFMAX, ext.shape[1]
    branches, width = kbuf.shape[0], kbuf.shape[2]
    reach = OFFMAX
    first = rank % 2
    second = 1 - first

    def at(energy, slice_):
        return {"energy": energy, "cuts": slice_}

    has = (rank > 0, rank < n_energy - 1)
    beside = (jnp.maximum(rank - 1, 0), jnp.minimum(rank + 1, n_energy - 1))
    if slots == 1:
        partners = [(1, 1, 1 - cut, None, 2 - 2 * cut)]
    elif slots == 2:
        partners = [
            (1, 2, jnp.maximum(cut - 1, 0), cut > 0, 0),
            (2, 1, jnp.minimum(cut + 1, n_cuts - 1), cut < n_cuts - 1, 2),
        ]
    else:
        partners = []

    def when(cond, do):
        if cond is None:
            do()
        else:
            pl.when(cond)(do)

    def exists(p):
        return jnp.where(p == 0, rank, n_energy - 1 - rank) > 0

    def toward(p):
        return jnp.clip(rank + 2 * p - 1, 0, n_energy - 1)

    def source(p):
        return (count - reach) * p + reach

    def landing(p):
        return (count + reach) * (1 - p)

    def edge(p, c):
        return green.at[pl.ds((count - reach) * p, reach), 0, c]

    def own_copy(p, c):
        return pltpu.make_async_remote_copy(
            src_ref=edge(p, c),
            dst_ref=ext.at[0, c, pl.ds(landing(p), reach)],
            send_sem=own_send.at[p, c], recv_sem=own_recv.at[p, c],
            device_id=at(toward(p), cut), device_id_type=MESH)

    def relay_copy(slot, p, c):
        return pltpu.make_async_remote_copy(
            src_ref=ext.at[slot, c, pl.ds(source(p), reach)],
            dst_ref=ext.at[slot, c, pl.ds(landing(p), reach)],
            send_sem=relay_send.at[slot - 1, p, c], recv_sem=relay_recv.at[slot - 1, p, c],
            device_id=at(toward(p), cut), device_id_type=MESH)

    def x_copy(there, partner, p, c):
        return pltpu.make_async_remote_copy(
            src_ref=edge(p, c),
            dst_ref=ext.at[there, c, pl.ds(source(p), reach)],
            send_sem=x_send.at[there - 1, p, c], recv_sem=x_recv.at[there - 1, p, c],
            device_id=at(rank, partner), device_id_type=MESH)

    barrier = pltpu.get_barrier_semaphore()
    for p in range(2):
        pl.when(has[p])(functools.partial(
            pl.semaphore_signal, barrier, inc=1, device_id=at(beside[p], cut), device_id_type=MESH))
    for here, there, partner, cond, side in partners:
        when(cond, functools.partial(
            pl.semaphore_signal, barrier, inc=1, device_id=at(rank, partner), device_id_type=MESH))

    local = [pltpu.make_async_copy(green.at[:, 0, c], ext.at[0, c, pl.ds(reach, count)], local_sem.at[c])
             for c in range(parts)]
    for c in range(parts):
        local[c].start()
    k_copy = pltpu.make_async_copy(coupling.at[:, :, 0], kbuf, k_sem)
    k_copy.start()
    small = [pltpu.make_async_copy(offsets_in, offsets, small_sem.at[0]),
             pltpu.make_async_copy(occupation_in, occupation, small_sem.at[1])]
    for copy in small:
        copy.start()

    peers = sum(flag.astype(jnp.int32) for flag in has)
    for here, there, partner, cond, side in partners:
        peers = peers + (1 if cond is None else cond.astype(jnp.int32))
    pl.semaphore_wait(barrier, peers)

    order = [(0, 0)]
    for c in range(1, parts):
        order += [(0, c), (1, c - 1)]
    order += [(1, parts - 1)]
    for which, c in order:
        p = (first, second)[which]
        for here, there, partner, cond, side in partners:
            when(cond, lambda: x_copy(there, partner, p, c).start())
        if which == 0:
            for q in (first, second):
                pl.when(exists(q))(lambda: own_copy(q, c).start())

    @pl.when(rank == 0)
    def _():
        ext[:, :, pl.ds(0, reach)] = jnp.zeros((slots + 1, parts, reach, width, width), ext.dtype)

    @pl.when(rank == n_energy - 1)
    def _():
        ext[:, :, pl.ds(count + reach, reach)] = jnp.zeros((slots + 1, parts, reach, width, width), ext.dtype)

    k_copy.wait()
    for copy in small + local:
        copy.wait()
    for s in range(kbuf.shape[1]):
        for b in range(branches):
            kt[s, b * width:(b + 1) * width, :] = kbuf[b, s].T

    def forward(which, c):
        p = (first, second)[which]
        for here, there, partner, cond, side in partners:
            def go():
                x_copy(here, partner, p, c).wait_recv()
                pl.when(exists(p))(lambda: relay_copy(here, p, c).start())
            when(cond, go)

    def own_ready(c):
        for p in range(2):
            pl.when(has[p])(lambda: own_copy(1 - p, c).wait_recv())

    steps = parts * (slots + 1)
    last = 2 * parts - 2
    plan = {}
    for position, item in enumerate(order if partners else []):
        plan.setdefault(min(position, last), []).append(item)

    def compute(slot, side, c):
        values = [ext[slot, c, e].astype(jnp.float32) for e in range(count + 2 * reach)]
        lefts = []
        for b in range(branches):
            n = occupation[b]
            w = offsets[b]
            lesser = c < parts // 2
            lower = jnp.where(lesser, n, n + 1.0)
            upper = jnp.where(lesser, n + 1.0, n)
            low = [jnp.where(w == d, lower, 0.0) for d in range(1, reach + 1)]
            up = [jnp.where(w == d, upper, 0.0) for d in range(1, reach + 1)]
            mixed = []
            for e in range(count):
                total = None
                for d in range(1, reach + 1):
                    term = low[d - 1] * values[reach + e - d] + up[d - 1] * values[reach + e + d]
                    total = term if total is None else total + term
                mixed.append(total.astype(jnp.bfloat16))
            lefts.append(jnp.dot(kbuf[b, side], jnp.concatenate(mixed, axis=1),
                                 preferred_element_type=jnp.float32).astype(jnp.bfloat16))
        rows = [jnp.concatenate([left[:, e * width:(e + 1) * width] for left in lefts], axis=1)
                for e in range(count)]
        return jnp.dot(jnp.concatenate(rows, axis=0), kt[side], preferred_element_type=jnp.float32)

    def step(t, carry):
        slot = t // parts
        c = t % parts
        for k, todo in plan.items():
            @pl.when(t == k)
            def _():
                for which, part in todo:
                    forward(which, part)

        @pl.when(slot == 0)
        def _():
            own_ready(c)

        runs = slot == 0
        side = jnp.where(slot == 0, 1, 0)
        for here, there, partner, cond, which_side in partners:
            side = jnp.where(slot == here, which_side, side)
            mine = slot == here
            if cond is not None:
                mine = jnp.logical_and(mine, cond)
            runs = jnp.logical_or(runs, mine)

            @pl.when(mine)
            def _():
                for p in range(2):
                    pl.when(has[p])(lambda: relay_copy(here, 1 - p, c).wait_recv())

        def work():
            sums = compute(slot, side, c)

            @pl.when(slot == 0)
            def _():
                for e in range(count):
                    acc[c, e] = sums[e * width:(e + 1) * width]

            @pl.when(slot > 0)
            def _():
                for e in range(count):
                    acc[c, e] += sums[e * width:(e + 1) * width]

        if slots == 2:
            pl.when(runs)(work)
        else:
            work()

        return carry

    lax.fori_loop(0, steps, step, 0)

    for c in range(parts):
        for p in range(2):
            pl.when(has[p])(lambda: own_copy(p, c).wait_send())
            for here, there, partner, cond, side in partners:
                when(cond, lambda: x_copy(there, partner, p, c).wait_send())
                both = has[p] if cond is None else jnp.logical_and(cond, has[p])
                pl.when(both)(lambda: relay_copy(here, p, c).wait_send())


def write_out(sums, out, sem):
    copies = [pltpu.make_async_copy(sums.at[c], out.at[:, 0, c], sem.at[c]) for c in range(sums.shape[0])]
    for copy in copies:
        copy.start()
    for copy in copies:
        copy.wait()


def body(n_energy, n_cuts, green, offsets, occupation, coupling):
    count, slices, parts, width, _ = green.shape
    branches, sides = coupling.shape[:2]
    assert slices == 1 and count == 2 * OFFMAX
    slots = min(n_cuts - 1, 2)
    sems = max(slots, 1)
    dma = pltpu.SemaphoreType.DMA
    sums = pl.pallas_call(
        functools.partial(kernel, n_energy, n_cuts, slots),
        out_shape=pltpu.VMEM((parts, count, width, width), jnp.float32),
        in_specs=[
            pl.BlockSpec(memory_space=pl.ANY),
            pl.BlockSpec(memory_space=pl.ANY),
            pl.BlockSpec(memory_space=pl.ANY),
            pl.BlockSpec(memory_space=pl.ANY),
        ],
        out_specs=pl.BlockSpec(memory_space=pltpu.VMEM),
        scratch_shapes=[
            pltpu.SMEM(offsets.shape, offsets.dtype),
            pltpu.SMEM(occupation.shape, occupation.dtype),
            pltpu.VMEM((slots + 1, parts, count + 2 * OFFMAX, width, width), jnp.bfloat16),
            pltpu.VMEM((branches, sides, width, width), jnp.bfloat16),
            pltpu.VMEM((sides, branches * width, width), jnp.bfloat16),
            dma((2,)),
            dma((parts,)),
            dma,
            dma((2, parts)),
            dma((2, parts)),
            dma((sems, 2, parts)),
            dma((sems, 2, parts)),
            dma((sems, 2, parts)),
            dma((sems, 2, parts)),
        ],
        compiler_params=pltpu.CompilerParams(collective_id=0, has_side_effects=True),
    )(offsets, occupation, green, coupling)
    return pl.pallas_call(
        write_out,
        out_shape=jax.ShapeDtypeStruct(green.shape, jnp.float32),
        in_specs=[pl.BlockSpec(memory_space=pltpu.VMEM)],
        out_specs=pl.BlockSpec(memory_space=pl.ANY),
        scratch_shapes=[dma((parts,))],
    )(pltpu.with_memory_space_constraint(sums, pltpu.VMEM))


def targets(values, k, k_t, lower, upper, near):
    width, reach = k_t.shape[1], OFFMAX
    count = len(values) - 2 * reach
    lefts = []
    for b in range(k.shape[0]):
        mixed = []
        for e in range(reach, reach + count):
            below = jnp.where(near[b], values[e - 1], values[e - 2])
            above = jnp.where(near[b], values[e + 1], values[e + 2])
            mixed.append((lower[b] * below + upper[b] * above).astype(jnp.bfloat16))
        lefts.append(jnp.dot(k[b], jnp.concatenate(mixed, axis=1),
                             preferred_element_type=jnp.float32).astype(jnp.bfloat16))
    return [jnp.dot(jnp.concatenate([left[:, e * width:(e + 1) * width] for left in lefts], axis=1), k_t[...],
                    preferred_element_type=jnp.float32) for e in range(count)]


def pair_kernel(n_energy, offsets_in, occupation_in, green, coupling, acc, far, kbuf, kt, scales,
                offsets, occupation, own, edge_out, edge_in, local_sem,
                reply_x, reply_e, send, x_recv, own_recv, relay_recv, edge_recv):
    rank = lax.axis_index("energy")
    cut = lax.axis_index("cuts")
    reach = OFFMAX
    count, parts, width = own.shape[0] - 2 * reach, own.shape[1], own.shape[2]
    branches = kbuf.shape[1]
    outer = rank % 2
    inner = 1 - outer
    has_outer = jnp.where(outer == 0, rank, n_energy - 1 - rank) > 0
    early = jnp.where(has_outer, outer, inner)
    late = 1 - early
    core_peer = {"energy": rank + 1 - 2 * outer, "cuts": cut}
    chip_peer = {"energy": jnp.clip(rank - 1 + 2 * outer, 0, n_energy - 1), "cuts": cut}
    slice_peer = {"energy": rank, "cuts": 1 - cut}
    told = (rank + cut) % 2 == 0
    tells = (rank + cut) % 2 == 1

    def own_at(p):
        return pl.ds(reach + (count - reach) * p, reach)

    def halo_at(p):
        return pl.ds((count + reach) * p, reach)

    def edge_at(p):
        return pl.ds((count - reach) * p, reach)

    def x_copy(p, c):
        return pltpu.make_async_remote_copy(
            src_ref=green.at[edge_at(p), 0, c], dst_ref=far.at[own_at(p), c],
            send_sem=send.at[0], recv_sem=x_recv.at[p, c], device_id=slice_peer, device_id_type=MESH)

    def own_copy():
        return pltpu.make_async_remote_copy(
            src_ref=green.at[edge_at(inner), 0], dst_ref=own.at[halo_at(outer)],
            send_sem=send.at[1], recv_sem=own_recv, device_id=core_peer, device_id_type=MESH)

    def relay_copy(c):
        return pltpu.make_async_remote_copy(
            src_ref=far.at[own_at(inner), c], dst_ref=far.at[halo_at(outer), c],
            send_sem=send.at[2], recv_sem=relay_recv.at[c], device_id=core_peer, device_id_type=MESH)

    def edge_copy(c):
        return pltpu.make_async_remote_copy(
            src_ref=edge_out.at[c], dst_ref=edge_in.at[c],
            send_sem=send.at[3], recv_sem=edge_recv.at[c], device_id=chip_peer, device_id_type=MESH)

    def signal(sem, device):
        pl.semaphore_signal(sem, inc=1, device_id=device, device_id_type=MESH)

    barrier = pltpu.get_barrier_semaphore()

    @pl.when(tells)
    def _():
        signal(barrier, slice_peer)

    @pl.when(told)
    def _():
        signal(barrier, core_peer)

    @pl.when(jnp.logical_and(told, has_outer))
    def _():
        signal(barrier, chip_peer)

    @pl.when(told)
    def _():
        pl.semaphore_wait(barrier, 1)
        signal(reply_x, slice_peer)

    @pl.when(tells)
    def _():
        pl.semaphore_wait(reply_x, 1)

    held_back = jnp.logical_and(outer == 1, rank > 1)
    for c in range(parts):
        x_copy(early, c).start()

    @pl.when(jnp.logical_not(held_back))
    def _():
        for c in range(parts):
            x_copy(late, c).start()

    def release(point):
        for c in range(parts):
            at = jnp.where(cut == 0, HOLD[0][c], HOLD[1][c])
            pl.when(jnp.logical_and(held_back, point == at))(lambda: x_copy(late, c).start())

    local = [pltpu.make_async_copy(green.at[:, 0], own.at[pl.ds(reach, count)], local_sem.at[0]),
             pltpu.make_async_copy(coupling.at[:, 1, 0], kbuf.at[0], local_sem.at[1]),
             pltpu.make_async_copy(coupling.at[:, 2 - 2 * cut, 0], kbuf.at[1], local_sem.at[2]),
             pltpu.make_async_copy(offsets_in, offsets, local_sem.at[3]),
             pltpu.make_async_copy(occupation_in, occupation, local_sem.at[4])]
    for copy in local:
        copy.start()

    @pl.when(tells)
    def _():
        pl.semaphore_wait(barrier, 1 + has_outer.astype(jnp.int32))
        signal(reply_e.at[0], core_peer)

    @pl.when(jnp.logical_and(tells, has_outer))
    def _():
        signal(reply_e.at[1], chip_peer)

    @pl.when(told)
    def _():
        pl.semaphore_wait(reply_e.at[0], 1)

    own_copy().start()

    own[halo_at(outer)] = jnp.zeros((reach, parts, width, width), own.dtype)
    far[halo_at(outer)] = jnp.zeros((reach, parts, width, width), far.dtype)
    for copy in local:
        copy.wait()
    for s in range(2):
        for b in range(branches):
            kt[s, b * width:(b + 1) * width, :] = kbuf[s, b].T

    @pl.when(jnp.logical_and(told, has_outer))
    def _():
        pl.semaphore_wait(reply_e.at[1], 1)

    own_copy().wait_recv()

    def weights(c):
        lesser = c < parts // 2
        lower = [jnp.where(lesser, occupation[b], occupation[b] + 1.0) for b in range(branches)]
        upper = [jnp.where(lesser, occupation[b] + 1.0, occupation[b]) for b in range(branches)]
        return lower, upper, [offsets[b] == 1 for b in range(branches)]

    def unit(blocks, s, c):
        values = [blocks[e, c].astype(jnp.float32) for e in range(count + 2 * reach)]
        return targets(values, kbuf.at[s], kt.at[s], *weights(c))

    def edge(c):
        lower, upper, near = weights(c)
        lefts = []
        for s, blocks in enumerate((own, far)):
            first = blocks[reach + (count - 1) * outer, c].astype(jnp.float32)
            second = blocks[reach + 1 + (count - 3) * outer, c].astype(jnp.float32)
            for b in range(branches):
                gain = jnp.where(outer == 0, upper[b], lower[b])
                one = gain * jnp.where(near[b], first, second)
                two = jnp.where(near[b], 0.0, gain) * first
                both = jnp.concatenate([one.astype(jnp.bfloat16), two.astype(jnp.bfloat16)], axis=1)
                lefts.append(jnp.dot(kbuf[s, b], both, preferred_element_type=jnp.float32).astype(jnp.bfloat16))
        rows = [jnp.concatenate([left[:, e * width:(e + 1) * width] for left in lefts], axis=1)
                for e in range(reach)]
        sums = jnp.dot(jnp.concatenate(rows, axis=0), kt[...].reshape(2 * branches * width, width),
                       preferred_element_type=jnp.float32).astype(edge_out.dtype)
        for e in range(reach):
            edge_out[c, e] = sums[e * width:(e + 1) * width]

    def first_half(c, carry):
        x_copy(early, c).wait_recv()
        release(c)

        @pl.when(has_outer)
        def _():
            edge(c)

        @pl.when(jnp.logical_not(has_outer))
        def _():
            relay_copy(c).start()

        sums = unit(own, 0, c)
        for e in range(count):
            acc[e, c] = sums[e]
        pl.when(has_outer)(lambda: edge_copy(c).start())
        return carry

    lax.fori_loop(0, parts, first_half, 0)

    def arrived(c):
        x_copy(late, c).wait_recv()
        release(parts + c)
        pl.when(has_outer)(lambda: relay_copy(c).start())

    def halo(c):
        relay_copy(c).wait_recv()

        @pl.when(has_outer)
        def _():
            edge_copy(c).wait_recv()
            acc[(count - 1) * outer, c] += edge_in[c, 0].astype(jnp.float32)
            acc[1 + (count - 3) * outer, c] += edge_in[c, 1].astype(jnp.float32)

    pl.when(has_outer)(lambda: arrived(0))

    def second_half(c, carry):
        pl.when(has_outer)(lambda: arrived(c + 1))
        pl.when(jnp.logical_not(has_outer))(lambda: arrived(c))
        halo(c)
        sums = unit(far, 1, c)
        for e in range(count):
            acc[e, c] += sums[e]
        return carry

    lax.fori_loop(0, parts - 1, second_half, 0)
    lower, upper, near = weights(parts - 1)
    for b in range(branches):
        for i, value in enumerate((lower[b], upper[b], jnp.where(near[b], 1.0, 0.0))):
            scales[i, pl.ds(b, 1)] = jnp.full((1, width), value, jnp.float32)
    pl.when(jnp.logical_not(has_outer))(lambda: arrived(parts - 1))
    halo(parts - 1)

    def sent(ref, n):
        pltpu.make_async_copy(ref, ref, send.at[n]).wait()

    sent(far.at[pl.ds(reach, count)], 0)
    sent(own.at[pl.ds(0, reach)], 1)
    sent(far.at[pl.ds(0, reach)], 2)
    pl.when(has_outer)(lambda: sent(edge_out, 3))


def pair_finish(sums, far, kbuf, kt, scales, out, held, write, last_write):
    count, parts = sums.shape[:2]
    last = parts - 1
    copies = [pltpu.make_async_copy(sums.at[:, c], out.at[:, 0, c], write.at[c]) for c in range(last)]
    for copy in copies:
        copy.start()
    branches = range(kbuf.shape[1])
    values = [far[e, last].astype(jnp.float32) for e in range(far.shape[0])]
    rows = [[scales[i, pl.ds(b, 1)] for b in branches] for i in range(3)]
    terms = targets(values, kbuf.at[1], kt.at[1], rows[0], rows[1], [row > 0.5 for row in rows[2]])
    for e in range(count):
        held[e] = sums[e, last] + terms[e]
        copies.append(pltpu.make_async_copy(held.at[e], out.at[e, 0, last], last_write.at[e]))
        copies[-1].start()
    for copy in copies:
        copy.wait()


def pair_body(n_energy, green, offsets, occupation, coupling):
    count, slices, parts, width, _ = green.shape
    branches = coupling.shape[0]
    assert slices == 1 and count == 2 * OFFMAX
    dma = pltpu.SemaphoreType.DMA
    regular = pltpu.SemaphoreType.REGULAR
    vmem = pl.BlockSpec(memory_space=pltpu.VMEM)
    made = pl.pallas_call(
        functools.partial(pair_kernel, n_energy),
        out_shape=[
            pltpu.VMEM((count, parts, width, width), jnp.float32),
            pltpu.VMEM((count + 2 * OFFMAX, parts, width, width), jnp.bfloat16),
            pltpu.VMEM((2, branches, width, width), jnp.bfloat16),
            pltpu.VMEM((2, branches * width, width), jnp.bfloat16),
            pltpu.VMEM((3, branches, width), jnp.float32),
        ],
        in_specs=[pl.BlockSpec(memory_space=pl.ANY)] * 4,
        out_specs=[vmem] * 5,
        scratch_shapes=[
            pltpu.SMEM(offsets.shape, offsets.dtype),
            pltpu.SMEM(occupation.shape, occupation.dtype),
            pltpu.VMEM((count + 2 * OFFMAX, parts, width, width), jnp.bfloat16),
            pltpu.VMEM((parts, OFFMAX, width, width), jnp.bfloat16),
            pltpu.VMEM((parts, OFFMAX, width, width), jnp.bfloat16),
            dma((5,)),
            regular,
            regular((2,)),
            dma((4,)),
            dma((2, parts)),
            dma,
            dma((parts,)),
            dma((parts,)),
        ],
        compiler_params=pltpu.CompilerParams(collective_id=0, has_side_effects=True),
    )(offsets, occupation, green, coupling)
    return pl.pallas_call(
        pair_finish,
        out_shape=jax.ShapeDtypeStruct(green.shape, jnp.float32),
        in_specs=[vmem] * 5,
        out_specs=pl.BlockSpec(memory_space=pl.ANY),
        scratch_shapes=[pltpu.VMEM((count, width, width), jnp.float32), dma((parts,)), dma((count,))],
    )(*[pltpu.with_memory_space_constraint(x, pltpu.VMEM) for x in made])


def solution(mesh):
    sizes = dict(mesh.shape)
    in_specs = (P("energy", "cuts", None, None, None), P(), P(), P(None, None, "cuts", None, None))
    out_specs = P("energy", "cuts", None, None, None)
    if sizes["cuts"] == 2 and sizes["energy"] % 2 == 0:
        step = functools.partial(pair_body, sizes["energy"])
    else:
        step = functools.partial(body, sizes["energy"], sizes["cuts"])
    return jax.shard_map(step, mesh=mesh, in_specs=in_specs, out_specs=out_specs, check_vma=False)
```

```python
import functools
import jax
import jax.numpy as jnp
from jax import lax
from jax.experimental import pallas as pl
from jax.experimental.pallas import tpu as pltpu
from jax.sharding import PartitionSpec as P

OFFMAX = 2
HOLD = ((3, 3, 4, 5), (2, 2, 3, 3))
MESH = pl.DeviceIdType.MESH


def kernel(n_energy, n_cuts, slots, offsets_in, occupation_in, green, coupling, acc,
           offsets, occupation, ext, kbuf, kt, small_sem, local_sem, k_sem,
           own_send, own_recv, x_send, x_recv, relay_send, relay_recv):
    rank = lax.axis_index("energy")
    cut = lax.axis_index("cuts")
    count, parts = ext.shape[2] - 2 * OFFMAX, ext.shape[1]
    branches, width = kbuf.shape[0], kbuf.shape[2]
    reach = OFFMAX
    first = rank % 2
    second = 1 - first

    def at(energy, slice_):
        return {"energy": energy, "cuts": slice_}

    has = (rank > 0, rank < n_energy - 1)
    beside = (jnp.maximum(rank - 1, 0), jnp.minimum(rank + 1, n_energy - 1))
    if slots == 1:
        partners = [(1, 1, 1 - cut, None, 2 - 2 * cut)]
    elif slots == 2:
        partners = [
            (1, 2, jnp.maximum(cut - 1, 0), cut > 0, 0),
            (2, 1, jnp.minimum(cut + 1, n_cuts - 1), cut < n_cuts - 1, 2),
        ]
    else:
        partners = []

    def when(cond, do):
        if cond is None:
            do()
        else:
            pl.when(cond)(do)

    def exists(p):
        return jnp.where(p == 0, rank, n_energy - 1 - rank) > 0

    def toward(p):
        return jnp.clip(rank + 2 * p - 1, 0, n_energy - 1)

    def source(p):
        return (count - reach) * p + reach

    def landing(p):
        return (count + reach) * (1 - p)

    def edge(p, c):
        return green.at[pl.ds((count - reach) * p, reach), 0, c]

    def own_copy(p, c):
        return pltpu.make_async_remote_copy(
            src_ref=edge(p, c),
            dst_ref=ext.at[0, c, pl.ds(landing(p), reach)],
            send_sem=own_send.at[p, c], recv_sem=own_recv.at[p, c],
            device_id=at(toward(p), cut), device_id_type=MESH)

    def relay_copy(slot, p, c):
        return pltpu.make_async_remote_copy(
            src_ref=ext.at[slot, c, pl.ds(source(p), reach)],
            dst_ref=ext.at[slot, c, pl.ds(landing(p), reach)],
            send_sem=relay_send.at[slot - 1, p, c], recv_sem=relay_recv.at[slot - 1, p, c],
            device_id=at(toward(p), cut), device_id_type=MESH)

    def x_copy(there, partner, p, c):
        return pltpu.make_async_remote_copy(
            src_ref=edge(p, c),
            dst_ref=ext.at[there, c, pl.ds(source(p), reach)],
            send_sem=x_send.at[there - 1, p, c], recv_sem=x_recv.at[there - 1, p, c],
            device_id=at(rank, partner), device_id_type=MESH)

    barrier = pltpu.get_barrier_semaphore()
    for p in range(2):
        pl.when(has[p])(functools.partial(
            pl.semaphore_signal, barrier, inc=1, device_id=at(beside[p], cut), device_id_type=MESH))
    for here, there, partner, cond, side in partners:
        when(cond, functools.partial(
            pl.semaphore_signal, barrier, inc=1, device_id=at(rank, partner), device_id_type=MESH))

    local = [pltpu.make_async_copy(green.at[:, 0, c], ext.at[0, c, pl.ds(reach, count)], local_sem.at[c])
             for c in range(parts)]
    for c in range(parts):
        local[c].start()
    k_copy = pltpu.make_async_copy(coupling.at[:, :, 0], kbuf, k_sem)
    k_copy.start()
    small = [pltpu.make_async_copy(offsets_in, offsets, small_sem.at[0]),
             pltpu.make_async_copy(occupation_in, occupation, small_sem.at[1])]
    for copy in small:
        copy.start()

    peers = sum(flag.astype(jnp.int32) for flag in has)
    for here, there, partner, cond, side in partners:
        peers = peers + (1 if cond is None else cond.astype(jnp.int32))
    pl.semaphore_wait(barrier, peers)

    order = [(0, 0)]
    for c in range(1, parts):
        order += [(0, c), (1, c - 1)]
    order += [(1, parts - 1)]
    for which, c in order:
        p = (first, second)[which]
        for here, there, partner, cond, side in partners:
            when(cond, lambda: x_copy(there, partner, p, c).start())
        if which == 0:
            for q in (first, second):
                pl.when(exists(q))(lambda: own_copy(q, c).start())

    @pl.when(rank == 0)
    def _():
        ext[:, :, pl.ds(0, reach)] = jnp.zeros((slots + 1, parts, reach, width, width), ext.dtype)

    @pl.when(rank == n_energy - 1)
    def _():
        ext[:, :, pl.ds(count + reach, reach)] = jnp.zeros((slots + 1, parts, reach, width, width), ext.dtype)

    k_copy.wait()
    for copy in small + local:
        copy.wait()
    for s in range(kbuf.shape[1]):
        for b in range(branches):
            kt[s, b * width:(b + 1) * width, :] = kbuf[b, s].T

    def forward(which, c):
        p = (first, second)[which]
        for here, there, partner, cond, side in partners:
            def go():
                x_copy(here, partner, p, c).wait_recv()
                pl.when(exists(p))(lambda: relay_copy(here, p, c).start())
            when(cond, go)

    def own_ready(c):
        for p in range(2):
            pl.when(has[p])(lambda: own_copy(1 - p, c).wait_recv())

    steps = parts * (slots + 1)
    last = 2 * parts - 2
    plan = {}
    for position, item in enumerate(order if partners else []):
        plan.setdefault(min(position, last), []).append(item)

    def compute(slot, side, c):
        values = [ext[slot, c, e].astype(jnp.float32) for e in range(count + 2 * reach)]
        lefts = []
        for b in range(branches):
            n = occupation[b]
            w = offsets[b]
            lesser = c < parts // 2
            lower = jnp.where(lesser, n, n + 1.0)
            upper = jnp.where(lesser, n + 1.0, n)
            low = [jnp.where(w == d, lower, 0.0) for d in range(1, reach + 1)]
            up = [jnp.where(w == d, upper, 0.0) for d in range(1, reach + 1)]
            mixed = []
            for e in range(count):
                total = None
                for d in range(1, reach + 1):
                    term = low[d - 1] * values[reach + e - d] + up[d - 1] * values[reach + e + d]
                    total = term if total is None else total + term
                mixed.append(total.astype(jnp.bfloat16))
            lefts.append(jnp.dot(kbuf[b, side], jnp.concatenate(mixed, axis=1),
                                 preferred_element_type=jnp.float32).astype(jnp.bfloat16))
        rows = [jnp.concatenate([left[:, e * width:(e + 1) * width] for left in lefts], axis=1)
                for e in range(count)]
        return jnp.dot(jnp.concatenate(rows, axis=0), kt[side], preferred_element_type=jnp.float32)

    def step(t, carry):
        slot = t // parts
        c = t % parts
        for k, todo in plan.items():
            @pl.when(t == k)
            def _():
                for which, part in todo:
                    forward(which, part)

        @pl.when(slot == 0)
        def _():
            own_ready(c)

        runs = slot == 0
        side = jnp.where(slot == 0, 1, 0)
        for here, there, partner, cond, which_side in partners:
            side = jnp.where(slot == here, which_side, side)
            mine = slot == here
            if cond is not None:
                mine = jnp.logical_and(mine, cond)
            runs = jnp.logical_or(runs, mine)

            @pl.when(mine)
            def _():
                for p in range(2):
                    pl.when(has[p])(lambda: relay_copy(here, 1 - p, c).wait_recv())

        def work():
            sums = compute(slot, side, c)

            @pl.when(slot == 0)
            def _():
                for e in range(count):
                    acc[c, e] = sums[e * width:(e + 1) * width]

            @pl.when(slot > 0)
            def _():
                for e in range(count):
                    acc[c, e] += sums[e * width:(e + 1) * width]

        if slots == 2:
            pl.when(runs)(work)
        else:
            work()

        return carry

    lax.fori_loop(0, steps, step, 0)

    for c in range(parts):
        for p in range(2):
            pl.when(has[p])(lambda: own_copy(p, c).wait_send())
            for here, there, partner, cond, side in partners:
                when(cond, lambda: x_copy(there, partner, p, c).wait_send())
                both = has[p] if cond is None else jnp.logical_and(cond, has[p])
                pl.when(both)(lambda: relay_copy(here, p, c).wait_send())


def write_out(sums, out, sem):
    copies = [pltpu.make_async_copy(sums.at[c], out.at[:, 0, c], sem.at[c]) for c in range(sums.shape[0])]
    for copy in copies:
        copy.start()
    for copy in copies:
        copy.wait()


def body(n_energy, n_cuts, green, offsets, occupation, coupling):
    count, slices, parts, width, _ = green.shape
    branches, sides = coupling.shape[:2]
    assert slices == 1 and count == 2 * OFFMAX
    slots = min(n_cuts - 1, 2)
    sems = max(slots, 1)
    dma = pltpu.SemaphoreType.DMA
    sums = pl.pallas_call(
        functools.partial(kernel, n_energy, n_cuts, slots),
        out_shape=pltpu.VMEM((parts, count, width, width), jnp.float32),
        in_specs=[
            pl.BlockSpec(memory_space=pl.ANY),
            pl.BlockSpec(memory_space=pl.ANY),
            pl.BlockSpec(memory_space=pl.ANY),
            pl.BlockSpec(memory_space=pl.ANY),
        ],
        out_specs=pl.BlockSpec(memory_space=pltpu.VMEM),
        scratch_shapes=[
            pltpu.SMEM(offsets.shape, offsets.dtype),
            pltpu.SMEM(occupation.shape, occupation.dtype),
            pltpu.VMEM((slots + 1, parts, count + 2 * OFFMAX, width, width), jnp.bfloat16),
            pltpu.VMEM((branches, sides, width, width), jnp.bfloat16),
            pltpu.VMEM((sides, branches * width, width), jnp.bfloat16),
            dma((2,)),
            dma((parts,)),
            dma,
            dma((2, parts)),
            dma((2, parts)),
            dma((sems, 2, parts)),
            dma((sems, 2, parts)),
            dma((sems, 2, parts)),
            dma((sems, 2, parts)),
        ],
        compiler_params=pltpu.CompilerParams(collective_id=0, has_side_effects=True),
    )(offsets, occupation, green, coupling)
    return pl.pallas_call(
        write_out,
        out_shape=jax.ShapeDtypeStruct(green.shape, jnp.float32),
        in_specs=[pl.BlockSpec(memory_space=pltpu.VMEM)],
        out_specs=pl.BlockSpec(memory_space=pl.ANY),
        scratch_shapes=[dma((parts,))],
    )(pltpu.with_memory_space_constraint(sums, pltpu.VMEM))


def targets(values, k, k_t, lower, upper, near):
    width, reach = k_t.shape[1], OFFMAX
    count = len(values) - 2 * reach
    lefts = []
    for b in range(k.shape[0]):
        mixed = []
        for e in range(reach, reach + count):
            below = jnp.where(near[b], values[e - 1], values[e - 2])
            above = jnp.where(near[b], values[e + 1], values[e + 2])
            mixed.append((lower[b] * below + upper[b] * above).astype(jnp.bfloat16))
        lefts.append(jnp.dot(k[b], jnp.concatenate(mixed, axis=1),
                             preferred_element_type=jnp.float32).astype(jnp.bfloat16))
    return [jnp.dot(jnp.concatenate([left[:, e * width:(e + 1) * width] for left in lefts], axis=1), k_t[...],
                    preferred_element_type=jnp.float32) for e in range(count)]


def pair_kernel(n_energy, offsets_in, occupation_in, green, coupling, acc, far, kbuf, kt, scales,
                offsets, occupation, own, edge_out, edge_in, local_sem,
                reply_x, reply_e, send, x_recv, own_recv, relay_recv, edge_recv):
    rank = lax.axis_index("energy")
    cut = lax.axis_index("cuts")
    reach = OFFMAX
    count, parts, width = own.shape[0] - 2 * reach, own.shape[1], own.shape[2]
    branches, half = kbuf.shape[1], count // 2
    outer = rank % 2
    inner = 1 - outer
    has_outer = jnp.where(outer == 0, rank, n_energy - 1 - rank) > 0
    early = jnp.where(has_outer, outer, inner)
    late = 1 - early
    core_peer = {"energy": rank + 1 - 2 * outer, "cuts": cut}
    chip_peer = {"energy": jnp.clip(rank - 1 + 2 * outer, 0, n_energy - 1), "cuts": cut}
    slice_peer = {"energy": rank, "cuts": 1 - cut}
    told = (rank + cut) % 2 == 0
    tells = (rank + cut) % 2 == 1

    def own_at(p):
        return pl.ds(reach + (count - reach) * p, reach)

    def halo_at(p):
        return pl.ds((count + reach) * p, reach)

    def edge_at(p):
        return pl.ds((count - reach) * p, reach)

    def x_copy(p, c):
        return pltpu.make_async_remote_copy(
            src_ref=green.at[edge_at(p), 0, c], dst_ref=far.at[own_at(p), c],
            send_sem=send.at[0], recv_sem=x_recv.at[p, c], device_id=slice_peer, device_id_type=MESH)

    def own_copy():
        return pltpu.make_async_remote_copy(
            src_ref=green.at[edge_at(inner), 0], dst_ref=own.at[halo_at(outer)],
            send_sem=send.at[0], recv_sem=own_recv, device_id=core_peer, device_id_type=MESH)

    def relay_copy(c):
        return pltpu.make_async_remote_copy(
            src_ref=far.at[own_at(inner), c], dst_ref=far.at[halo_at(outer), c],
            send_sem=send.at[0], recv_sem=relay_recv.at[c], device_id=core_peer, device_id_type=MESH)

    def edge_copy(c):
        return pltpu.make_async_remote_copy(
            src_ref=edge_out.at[c], dst_ref=edge_in.at[c],
            send_sem=send.at[1], recv_sem=edge_recv, device_id=chip_peer, device_id_type=MESH)

    def signal(sem, device):
        pl.semaphore_signal(sem, inc=1, device_id=device, device_id_type=MESH)

    barrier = pltpu.get_barrier_semaphore()

    @pl.when(tells)
    def _():
        signal(barrier, slice_peer)

    @pl.when(told)
    def _():
        signal(barrier, core_peer)

    @pl.when(jnp.logical_and(told, has_outer))
    def _():
        signal(barrier, chip_peer)

    @pl.when(told)
    def _():
        pl.semaphore_wait(barrier, 1)
        signal(reply_x, slice_peer)

    @pl.when(tells)
    def _():
        pl.semaphore_wait(reply_x, 1)

    held_back = jnp.logical_and(outer == 1, rank > 1)
    for c in range(parts):
        x_copy(early, c).start()

    @pl.when(jnp.logical_not(held_back))
    def _():
        for c in range(parts):
            x_copy(late, c).start()

    def release(point):
        for c in range(parts):
            at = jnp.where(cut == 0, HOLD[0][c], HOLD[1][c])
            pl.when(jnp.logical_and(held_back, point == at))(lambda: x_copy(late, c).start())

    local = [pltpu.make_async_copy(green.at[:, 0], own.at[pl.ds(reach, count)], local_sem.at[0]),
             pltpu.make_async_copy(offsets_in, offsets, local_sem.at[1]),
             pltpu.make_async_copy(occupation_in, occupation, local_sem.at[2])]
    for copy in local:
        copy.start()
    pltpu.make_async_copy(coupling.at[:, 1, 0], kbuf.at[0], local_sem.at[3]).start()
    pltpu.make_async_copy(coupling.at[:, 2 - 2 * cut, 0], kbuf.at[1], local_sem.at[3]).start()

    def whole(ref, sem):
        pltpu.make_async_copy(ref, ref, sem).wait()

    @pl.when(tells)
    def _():
        pl.semaphore_wait(barrier, 1 + has_outer.astype(jnp.int32))
        signal(reply_e.at[0], core_peer)

    @pl.when(jnp.logical_and(tells, has_outer))
    def _():
        signal(reply_e.at[1], chip_peer)

    @pl.when(told)
    def _():
        pl.semaphore_wait(reply_e.at[0], 1)

    own_copy().start()

    own[halo_at(outer)] = jnp.zeros((reach, parts, width, width), own.dtype)
    far[halo_at(outer)] = jnp.zeros((reach, parts, width, width), far.dtype)
    whole(kbuf, local_sem.at[3])
    for copy in local:
        copy.wait()
    for s in range(2):
        for b in range(branches):
            kt[s, b * width:(b + 1) * width, :] = kbuf[s, b].T

    @pl.when(jnp.logical_and(told, has_outer))
    def _():
        pl.semaphore_wait(reply_e.at[1], 1)

    own_copy().wait_recv()

    def weights(c):
        lesser = c < parts // 2
        lower = [jnp.where(lesser, occupation[b], occupation[b] + 1.0) for b in range(branches)]
        upper = [jnp.where(lesser, occupation[b] + 1.0, occupation[b]) for b in range(branches)]
        return lower, upper, [offsets[b] == 1 for b in range(branches)]

    def unit(blocks, s, c, start=0, n=count):
        values = [blocks[start + e, c].astype(jnp.float32) for e in range(n + 2 * reach)]
        return targets(values, kbuf.at[s], kt.at[s], *weights(c))

    def edge(c):
        lower, upper, near = weights(c)
        lefts = []
        for s, blocks in enumerate((own, far)):
            first = blocks[reach + (count - 1) * outer, c].astype(jnp.float32)
            second = blocks[reach + 1 + (count - 3) * outer, c].astype(jnp.float32)
            for b in range(branches):
                gain = jnp.where(outer == 0, upper[b], lower[b])
                one = gain * jnp.where(near[b], first, second)
                two = jnp.where(near[b], 0.0, gain) * first
                both = jnp.concatenate([one.astype(jnp.bfloat16), two.astype(jnp.bfloat16)], axis=1)
                lefts.append(jnp.dot(kbuf[s, b], both, preferred_element_type=jnp.float32).astype(jnp.bfloat16))
        rows = [jnp.concatenate([left[:, e * width:(e + 1) * width] for left in lefts], axis=1)
                for e in range(reach)]
        sums = jnp.dot(jnp.concatenate(rows, axis=0), kt[...].reshape(2 * branches * width, width),
                       preferred_element_type=jnp.float32).astype(edge_out.dtype)
        for e in range(reach):
            edge_out[c, e] = sums[e * width:(e + 1) * width]

    def first_half(c, carry):
        x_copy(early, c).wait_recv()
        release(c)

        @pl.when(has_outer)
        def _():
            edge(c)

        @pl.when(jnp.logical_not(has_outer))
        def _():
            relay_copy(c).start()

        sums = unit(own, 0, c)
        for e in range(count):
            acc[e, c] = sums[e]
        pl.when(has_outer)(lambda: edge_copy(c).start())
        return carry

    lax.fori_loop(0, parts, first_half, 0)

    def arrived(c):
        x_copy(late, c).wait_recv()
        release(parts + c)
        pl.when(has_outer)(lambda: relay_copy(c).start())

    def add(jobs):
        for (c, start, n), made in zip(jobs, [unit(far, 1, *job) for job in jobs]):
            for e in range(n):
                acc[start + e, c] += made[e]

    pl.when(has_outer)(lambda: arrived(0))

    def second_half(c, carry):
        pl.when(has_outer)(lambda: arrived(c + 1))
        pl.when(jnp.logical_not(has_outer))(lambda: arrived(c))
        relay_copy(c).wait_recv()
        add([(c, 0, count)])
        return carry

    lax.fori_loop(0, parts - 2, second_half, 0)
    last = parts - 1
    lower, upper, near = weights(last)
    for b in range(branches):
        for i, value in enumerate((lower[b], upper[b], jnp.where(near[b], 1.0, 0.0))):
            scales[i, pl.ds(b, 1)] = jnp.full((1, width), value, jnp.float32)
    c = last - 1

    @pl.when(has_outer)
    def _():
        arrived(last)
        relay_copy(c).wait_recv()
        add([(c, 0, count), (last, half * outer, half)])

    @pl.when(jnp.logical_not(has_outer))
    def _():
        arrived(c)
        relay_copy(c).wait_recv()
        add([(c, 0, count)])

    @pl.when(has_outer)
    def _():
        whole(edge_in, edge_recv)
        for c in range(parts):
            acc[(count - 1) * outer, c] += edge_in[c, 0].astype(jnp.float32)
            acc[1 + (count - 3) * outer, c] += edge_in[c, 1].astype(jnp.float32)

    pl.when(jnp.logical_not(has_outer))(lambda: arrived(last))
    relay_copy(last).wait_recv()
    whole(own, send.at[0])
    pl.when(has_outer)(lambda: whole(edge_out, send.at[1]))


def pair_finish(n_energy, sums, far, kbuf, kt, scales, out, held, sem):
    rank = lax.axis_index("energy")
    count, parts = sums.shape[:2]
    last, half = parts - 1, count // 2
    outer = rank % 2
    has_outer = jnp.where(outer == 0, rank, n_energy - 1 - rank) > 0

    def write(source, start, n, c):
        pltpu.make_async_copy(source, out.at[pl.ds(start, n), 0, c], sem).start()

    for c in range(last):
        write(sums.at[:, c], 0, count, c)

    def add(start, n):
        values = [far[start + e, last].astype(jnp.float32) for e in range(n + 2 * OFFMAX)]
        rows = [[scales[i, pl.ds(b, 1)] for b in range(kbuf.shape[1])] for i in range(3)]
        made = targets(values, kbuf.at[1], kt.at[1], rows[0], rows[1], [row > 0.5 for row in rows[2]])
        for e in range(n):
            held[e] = sums[start + e, last] + made[e]
            write(held.at[pl.ds(e, 1)], start + e, 1, last)

    @pl.when(has_outer)
    def _():
        write(sums.at[pl.ds(half * outer, half), last], half * outer, half, last)
        add(half * (1 - outer), half)

    pl.when(jnp.logical_not(has_outer))(lambda: add(0, count))
    pltpu.make_async_copy(sums, sums, sem).wait()


def pair_body(n_energy, green, offsets, occupation, coupling):
    count, slices, parts, width, _ = green.shape
    branches = coupling.shape[0]
    assert slices == 1 and count == 2 * OFFMAX
    dma = pltpu.SemaphoreType.DMA
    regular = pltpu.SemaphoreType.REGULAR
    vmem = pl.BlockSpec(memory_space=pltpu.VMEM)
    made = pl.pallas_call(
        functools.partial(pair_kernel, n_energy),
        out_shape=[
            pltpu.VMEM((count, parts, width, width), jnp.float32),
            pltpu.VMEM((count + 2 * OFFMAX, parts, width, width), jnp.bfloat16),
            pltpu.VMEM((2, branches, width, width), jnp.bfloat16),
            pltpu.VMEM((2, branches * width, width), jnp.bfloat16),
            pltpu.VMEM((3, branches, width), jnp.float32),
        ],
        in_specs=[pl.BlockSpec(memory_space=pl.ANY)] * 4,
        out_specs=[vmem] * 5,
        scratch_shapes=[
            pltpu.SMEM(offsets.shape, offsets.dtype),
            pltpu.SMEM(occupation.shape, occupation.dtype),
            pltpu.VMEM((count + 2 * OFFMAX, parts, width, width), jnp.bfloat16),
            pltpu.VMEM((parts, OFFMAX, width, width), jnp.bfloat16),
            pltpu.VMEM((parts, OFFMAX, width, width), jnp.bfloat16),
            dma((4,)),
            regular,
            regular((2,)),
            dma((2,)),
            dma((2, parts)),
            dma,
            dma((parts,)),
            dma,
        ],
        compiler_params=pltpu.CompilerParams(collective_id=0, has_side_effects=True),
    )(offsets, occupation, green, coupling)
    return pl.pallas_call(
        functools.partial(pair_finish, n_energy),
        out_shape=jax.ShapeDtypeStruct(green.shape, jnp.float32),
        in_specs=[vmem] * 5,
        out_specs=pl.BlockSpec(memory_space=pl.ANY),
        scratch_shapes=[pltpu.VMEM((count, width, width), jnp.float32), dma],
    )(*[pltpu.with_memory_space_constraint(x, pltpu.VMEM) for x in made])


def solution(mesh):
    sizes = dict(mesh.shape)
    in_specs = (P("energy", "cuts", None, None, None), P(), P(), P(None, None, "cuts", None, None))
    out_specs = P("energy", "cuts", None, None, None)
    if sizes["cuts"] == 2 and sizes["energy"] % 2 == 0:
        step = functools.partial(pair_body, sizes["energy"])
    else:
        step = functools.partial(body, sizes["energy"], sizes["cuts"])
    return jax.shard_map(step, mesh=mesh, in_specs=in_specs, out_specs=out_specs, check_vma=False)
```

```python
import functools
import jax
import jax.numpy as jnp
from jax import lax
from jax.experimental import pallas as pl
from jax.experimental.pallas import tpu as pltpu
from jax.sharding import PartitionSpec as P

OFFMAX = 2
HOLD = ((3, 3, 4, 5), (2, 2, 3, 3))
MESH = pl.DeviceIdType.MESH


def kernel(n_energy, n_cuts, slots, offsets_in, occupation_in, green, coupling, acc,
           offsets, occupation, ext, kbuf, kt, small_sem, local_sem, k_sem,
           own_send, own_recv, x_send, x_recv, relay_send, relay_recv):
    rank = lax.axis_index("energy")
    cut = lax.axis_index("cuts")
    count, parts = ext.shape[2] - 2 * OFFMAX, ext.shape[1]
    branches, width = kbuf.shape[0], kbuf.shape[2]
    reach = OFFMAX
    first = rank % 2
    second = 1 - first

    def at(energy, slice_):
        return {"energy": energy, "cuts": slice_}

    has = (rank > 0, rank < n_energy - 1)
    beside = (jnp.maximum(rank - 1, 0), jnp.minimum(rank + 1, n_energy - 1))
    if slots == 1:
        partners = [(1, 1, 1 - cut, None, 2 - 2 * cut)]
    elif slots == 2:
        partners = [
            (1, 2, jnp.maximum(cut - 1, 0), cut > 0, 0),
            (2, 1, jnp.minimum(cut + 1, n_cuts - 1), cut < n_cuts - 1, 2),
        ]
    else:
        partners = []

    def when(cond, do):
        if cond is None:
            do()
        else:
            pl.when(cond)(do)

    def exists(p):
        return jnp.where(p == 0, rank, n_energy - 1 - rank) > 0

    def toward(p):
        return jnp.clip(rank + 2 * p - 1, 0, n_energy - 1)

    def source(p):
        return (count - reach) * p + reach

    def landing(p):
        return (count + reach) * (1 - p)

    def edge(p, c):
        return green.at[pl.ds((count - reach) * p, reach), 0, c]

    def own_copy(p, c):
        return pltpu.make_async_remote_copy(
            src_ref=edge(p, c),
            dst_ref=ext.at[0, c, pl.ds(landing(p), reach)],
            send_sem=own_send.at[p, c], recv_sem=own_recv.at[p, c],
            device_id=at(toward(p), cut), device_id_type=MESH)

    def relay_copy(slot, p, c):
        return pltpu.make_async_remote_copy(
            src_ref=ext.at[slot, c, pl.ds(source(p), reach)],
            dst_ref=ext.at[slot, c, pl.ds(landing(p), reach)],
            send_sem=relay_send.at[slot - 1, p, c], recv_sem=relay_recv.at[slot - 1, p, c],
            device_id=at(toward(p), cut), device_id_type=MESH)

    def x_copy(there, partner, p, c):
        return pltpu.make_async_remote_copy(
            src_ref=edge(p, c),
            dst_ref=ext.at[there, c, pl.ds(source(p), reach)],
            send_sem=x_send.at[there - 1, p, c], recv_sem=x_recv.at[there - 1, p, c],
            device_id=at(rank, partner), device_id_type=MESH)

    barrier = pltpu.get_barrier_semaphore()
    for p in range(2):
        pl.when(has[p])(functools.partial(
            pl.semaphore_signal, barrier, inc=1, device_id=at(beside[p], cut), device_id_type=MESH))
    for here, there, partner, cond, side in partners:
        when(cond, functools.partial(
            pl.semaphore_signal, barrier, inc=1, device_id=at(rank, partner), device_id_type=MESH))

    local = [pltpu.make_async_copy(green.at[:, 0, c], ext.at[0, c, pl.ds(reach, count)], local_sem.at[c])
             for c in range(parts)]
    for c in range(parts):
        local[c].start()
    k_copy = pltpu.make_async_copy(coupling.at[:, :, 0], kbuf, k_sem)
    k_copy.start()
    small = [pltpu.make_async_copy(offsets_in, offsets, small_sem.at[0]),
             pltpu.make_async_copy(occupation_in, occupation, small_sem.at[1])]
    for copy in small:
        copy.start()

    peers = sum(flag.astype(jnp.int32) for flag in has)
    for here, there, partner, cond, side in partners:
        peers = peers + (1 if cond is None else cond.astype(jnp.int32))
    pl.semaphore_wait(barrier, peers)

    order = [(0, 0)]
    for c in range(1, parts):
        order += [(0, c), (1, c - 1)]
    order += [(1, parts - 1)]
    for which, c in order:
        p = (first, second)[which]
        for here, there, partner, cond, side in partners:
            when(cond, lambda: x_copy(there, partner, p, c).start())
        if which == 0:
            for q in (first, second):
                pl.when(exists(q))(lambda: own_copy(q, c).start())

    @pl.when(rank == 0)
    def _():
        ext[:, :, pl.ds(0, reach)] = jnp.zeros((slots + 1, parts, reach, width, width), ext.dtype)

    @pl.when(rank == n_energy - 1)
    def _():
        ext[:, :, pl.ds(count + reach, reach)] = jnp.zeros((slots + 1, parts, reach, width, width), ext.dtype)

    k_copy.wait()
    for copy in small + local:
        copy.wait()
    for s in range(kbuf.shape[1]):
        for b in range(branches):
            kt[s, b * width:(b + 1) * width, :] = kbuf[b, s].T

    def forward(which, c):
        p = (first, second)[which]
        for here, there, partner, cond, side in partners:
            def go():
                x_copy(here, partner, p, c).wait_recv()
                pl.when(exists(p))(lambda: relay_copy(here, p, c).start())
            when(cond, go)

    def own_ready(c):
        for p in range(2):
            pl.when(has[p])(lambda: own_copy(1 - p, c).wait_recv())

    steps = parts * (slots + 1)
    last = 2 * parts - 2
    plan = {}
    for position, item in enumerate(order if partners else []):
        plan.setdefault(min(position, last), []).append(item)

    def compute(slot, side, c):
        values = [ext[slot, c, e].astype(jnp.float32) for e in range(count + 2 * reach)]
        lefts = []
        for b in range(branches):
            n = occupation[b]
            w = offsets[b]
            lesser = c < parts // 2
            lower = jnp.where(lesser, n, n + 1.0)
            upper = jnp.where(lesser, n + 1.0, n)
            low = [jnp.where(w == d, lower, 0.0) for d in range(1, reach + 1)]
            up = [jnp.where(w == d, upper, 0.0) for d in range(1, reach + 1)]
            mixed = []
            for e in range(count):
                total = None
                for d in range(1, reach + 1):
                    term = low[d - 1] * values[reach + e - d] + up[d - 1] * values[reach + e + d]
                    total = term if total is None else total + term
                mixed.append(total.astype(jnp.bfloat16))
            lefts.append(jnp.dot(kbuf[b, side], jnp.concatenate(mixed, axis=1),
                                 preferred_element_type=jnp.float32).astype(jnp.bfloat16))
        rows = [jnp.concatenate([left[:, e * width:(e + 1) * width] for left in lefts], axis=1)
                for e in range(count)]
        return jnp.dot(jnp.concatenate(rows, axis=0), kt[side], preferred_element_type=jnp.float32)

    def step(t, carry):
        slot = t // parts
        c = t % parts
        for k, todo in plan.items():
            @pl.when(t == k)
            def _():
                for which, part in todo:
                    forward(which, part)

        @pl.when(slot == 0)
        def _():
            own_ready(c)

        runs = slot == 0
        side = jnp.where(slot == 0, 1, 0)
        for here, there, partner, cond, which_side in partners:
            side = jnp.where(slot == here, which_side, side)
            mine = slot == here
            if cond is not None:
                mine = jnp.logical_and(mine, cond)
            runs = jnp.logical_or(runs, mine)

            @pl.when(mine)
            def _():
                for p in range(2):
                    pl.when(has[p])(lambda: relay_copy(here, 1 - p, c).wait_recv())

        def work():
            sums = compute(slot, side, c)

            @pl.when(slot == 0)
            def _():
                for e in range(count):
                    acc[c, e] = sums[e * width:(e + 1) * width]

            @pl.when(slot > 0)
            def _():
                for e in range(count):
                    acc[c, e] += sums[e * width:(e + 1) * width]

        if slots == 2:
            pl.when(runs)(work)
        else:
            work()

        return carry

    lax.fori_loop(0, steps, step, 0)

    for c in range(parts):
        for p in range(2):
            pl.when(has[p])(lambda: own_copy(p, c).wait_send())
            for here, there, partner, cond, side in partners:
                when(cond, lambda: x_copy(there, partner, p, c).wait_send())
                both = has[p] if cond is None else jnp.logical_and(cond, has[p])
                pl.when(both)(lambda: relay_copy(here, p, c).wait_send())


def write_out(sums, out, sem):
    copies = [pltpu.make_async_copy(sums.at[c], out.at[:, 0, c], sem.at[c]) for c in range(sums.shape[0])]
    for copy in copies:
        copy.start()
    for copy in copies:
        copy.wait()


def body(n_energy, n_cuts, green, offsets, occupation, coupling):
    count, slices, parts, width, _ = green.shape
    branches, sides = coupling.shape[:2]
    assert slices == 1 and count == 2 * OFFMAX
    slots = min(n_cuts - 1, 2)
    sems = max(slots, 1)
    dma = pltpu.SemaphoreType.DMA
    sums = pl.pallas_call(
        functools.partial(kernel, n_energy, n_cuts, slots),
        out_shape=pltpu.VMEM((parts, count, width, width), jnp.float32),
        in_specs=[
            pl.BlockSpec(memory_space=pl.ANY),
            pl.BlockSpec(memory_space=pl.ANY),
            pl.BlockSpec(memory_space=pl.ANY),
            pl.BlockSpec(memory_space=pl.ANY),
        ],
        out_specs=pl.BlockSpec(memory_space=pltpu.VMEM),
        scratch_shapes=[
            pltpu.SMEM(offsets.shape, offsets.dtype),
            pltpu.SMEM(occupation.shape, occupation.dtype),
            pltpu.VMEM((slots + 1, parts, count + 2 * OFFMAX, width, width), jnp.bfloat16),
            pltpu.VMEM((branches, sides, width, width), jnp.bfloat16),
            pltpu.VMEM((sides, branches * width, width), jnp.bfloat16),
            dma((2,)),
            dma((parts,)),
            dma,
            dma((2, parts)),
            dma((2, parts)),
            dma((sems, 2, parts)),
            dma((sems, 2, parts)),
            dma((sems, 2, parts)),
            dma((sems, 2, parts)),
        ],
        compiler_params=pltpu.CompilerParams(collective_id=0, has_side_effects=True),
    )(offsets, occupation, green, coupling)
    return pl.pallas_call(
        write_out,
        out_shape=jax.ShapeDtypeStruct(green.shape, jnp.float32),
        in_specs=[pl.BlockSpec(memory_space=pltpu.VMEM)],
        out_specs=pl.BlockSpec(memory_space=pl.ANY),
        scratch_shapes=[dma((parts,))],
    )(pltpu.with_memory_space_constraint(sums, pltpu.VMEM))


def targets(values, k, k_t, lower, upper, near):
    width, reach = k_t.shape[1], OFFMAX
    count = len(values) - 2 * reach
    lefts = []
    for b in range(k.shape[0]):
        mixed = []
        for e in range(reach, reach + count):
            below = jnp.where(near[b], values[e - 1], values[e - 2])
            above = jnp.where(near[b], values[e + 1], values[e + 2])
            mixed.append((lower[b] * below + upper[b] * above).astype(jnp.bfloat16))
        lefts.append(jnp.dot(k[b], jnp.concatenate(mixed, axis=1),
                             preferred_element_type=jnp.float32).astype(jnp.bfloat16))
    return [jnp.dot(jnp.concatenate([left[:, e * width:(e + 1) * width] for left in lefts], axis=1), k_t[...],
                    preferred_element_type=jnp.float32) for e in range(count)]


def pair_kernel(n_energy, offsets_in, occupation_in, green, coupling, acc, far, kbuf, kt, scales,
                offsets, occupation, own, edge_out, edge_in, local_sem,
                reply_x, reply_e, send, x_recv, own_recv, relay_recv, edge_recv):
    rank = lax.axis_index("energy")
    cut = lax.axis_index("cuts")
    reach = OFFMAX
    count, parts, width = own.shape[0] - 2 * reach, own.shape[1], own.shape[2]
    branches, half = kbuf.shape[1], count // 2
    outer = rank % 2
    inner = 1 - outer
    has_outer = jnp.where(outer == 0, rank, n_energy - 1 - rank) > 0
    early = jnp.where(has_outer, outer, inner)
    late = 1 - early
    core_peer = {"energy": rank + 1 - 2 * outer, "cuts": cut}
    chip_peer = {"energy": jnp.clip(rank - 1 + 2 * outer, 0, n_energy - 1), "cuts": cut}
    slice_peer = {"energy": rank, "cuts": 1 - cut}
    told = (rank + cut) % 2 == 0
    tells = (rank + cut) % 2 == 1

    def own_at(p):
        return pl.ds(reach + (count - reach) * p, reach)

    def halo_at(p):
        return pl.ds((count + reach) * p, reach)

    def edge_at(p):
        return pl.ds((count - reach) * p, reach)

    def x_copy(p, c):
        return pltpu.make_async_remote_copy(
            src_ref=green.at[edge_at(p), 0, c], dst_ref=far.at[own_at(p), c],
            send_sem=send.at[0], recv_sem=x_recv.at[p, c], device_id=slice_peer, device_id_type=MESH)

    def own_copy():
        return pltpu.make_async_remote_copy(
            src_ref=green.at[edge_at(inner), 0], dst_ref=own.at[halo_at(outer)],
            send_sem=send.at[0], recv_sem=own_recv, device_id=core_peer, device_id_type=MESH)

    def relay_copy(c):
        return pltpu.make_async_remote_copy(
            src_ref=far.at[own_at(inner), c], dst_ref=far.at[halo_at(outer), c],
            send_sem=send.at[0], recv_sem=relay_recv.at[c], device_id=core_peer, device_id_type=MESH)

    def edge_copy(c):
        return pltpu.make_async_remote_copy(
            src_ref=edge_out.at[c], dst_ref=edge_in.at[c],
            send_sem=send.at[1], recv_sem=edge_recv, device_id=chip_peer, device_id_type=MESH)

    def signal(sem, device):
        pl.semaphore_signal(sem, inc=1, device_id=device, device_id_type=MESH)

    barrier = pltpu.get_barrier_semaphore()

    @pl.when(tells)
    def _():
        signal(barrier, slice_peer)

    @pl.when(jnp.logical_and(told, cut == 0))
    def _():
        signal(barrier, core_peer)

    @pl.when(jnp.logical_and(jnp.logical_and(told, cut == 0), has_outer))
    def _():
        signal(barrier, chip_peer)

    @pl.when(told)
    def _():
        pl.semaphore_wait(barrier, 1)
        signal(reply_x, slice_peer)

    @pl.when(tells)
    def _():
        pl.semaphore_wait(reply_x, 1)

    held_back = jnp.logical_and(outer == 1, rank > 1)
    for c in range(parts):
        x_copy(early, c).start()

    @pl.when(jnp.logical_and(told, cut != 0))
    def _():
        signal(barrier, core_peer)

    @pl.when(jnp.logical_and(jnp.logical_and(told, cut != 0), has_outer))
    def _():
        signal(barrier, chip_peer)

    @pl.when(jnp.logical_not(held_back))
    def _():
        for c in range(parts):
            x_copy(late, c).start()

    def release(point):
        for c in range(parts):
            at = jnp.where(cut == 0, HOLD[0][c], HOLD[1][c])
            pl.when(jnp.logical_and(held_back, point == at))(lambda: x_copy(late, c).start())

    loads = [pltpu.make_async_copy(green.at[:, 0], own.at[pl.ds(reach, count)], local_sem.at[0]),
             pltpu.make_async_copy(coupling.at[:, 1, 0], kbuf.at[0], local_sem.at[0]),
             pltpu.make_async_copy(coupling.at[:, 2 - 2 * cut, 0], kbuf.at[1], local_sem.at[0])]
    local = [pltpu.make_async_copy(offsets_in, offsets, local_sem.at[1]),
             pltpu.make_async_copy(occupation_in, occupation, local_sem.at[2])]
    for copy in loads + local:
        copy.start()

    def whole(ref, sem):
        pltpu.make_async_copy(ref, ref, sem).wait()

    @pl.when(tells)
    def _():
        pl.semaphore_wait(barrier, 1 + has_outer.astype(jnp.int32))
        signal(reply_e.at[0], core_peer)

    @pl.when(jnp.logical_and(tells, has_outer))
    def _():
        signal(reply_e.at[1], chip_peer)

    @pl.when(told)
    def _():
        pl.semaphore_wait(reply_e.at[0], 1)

    own_copy().start()

    own[halo_at(outer)] = jnp.zeros((reach, parts, width, width), own.dtype)
    far[halo_at(outer)] = jnp.zeros((reach, parts, width, width), far.dtype)
    whole(own.at[pl.ds(0, count + 2 * branches // parts)], local_sem.at[0])
    for copy in local:
        copy.wait()
    for s in range(2):
        for b in range(branches):
            kt[s, b * width:(b + 1) * width, :] = kbuf[s, b].T

    @pl.when(jnp.logical_and(told, has_outer))
    def _():
        pl.semaphore_wait(reply_e.at[1], 1)

    own_copy().wait_recv()

    def weights(c):
        lesser = c < parts // 2
        lower = [jnp.where(lesser, occupation[b], occupation[b] + 1.0) for b in range(branches)]
        upper = [jnp.where(lesser, occupation[b] + 1.0, occupation[b]) for b in range(branches)]
        return lower, upper, [offsets[b] == 1 for b in range(branches)]

    def unit(blocks, s, c, start=0, n=count):
        values = [blocks[start + e, c].astype(jnp.float32) for e in range(n + 2 * reach)]
        return targets(values, kbuf.at[s], kt.at[s], *weights(c))

    def edge(c):
        lower, upper, near = weights(c)
        lefts = []
        for s, blocks in enumerate((own, far)):
            first = blocks[reach + (count - 1) * outer, c].astype(jnp.float32)
            second = blocks[reach + 1 + (count - 3) * outer, c].astype(jnp.float32)
            for b in range(branches):
                gain = jnp.where(outer == 0, upper[b], lower[b])
                one = gain * jnp.where(near[b], first, second)
                two = jnp.where(near[b], 0.0, gain) * first
                both = jnp.concatenate([one.astype(jnp.bfloat16), two.astype(jnp.bfloat16)], axis=1)
                lefts.append(jnp.dot(kbuf[s, b], both, preferred_element_type=jnp.float32).astype(jnp.bfloat16))
        rows = [jnp.concatenate([left[:, e * width:(e + 1) * width] for left in lefts], axis=1)
                for e in range(reach)]
        sums = jnp.dot(jnp.concatenate(rows, axis=0), kt[...].reshape(2 * branches * width, width),
                       preferred_element_type=jnp.float32).astype(edge_out.dtype)
        for e in range(reach):
            edge_out[c, e] = sums[e * width:(e + 1) * width]

    def first_half(c, carry):
        x_copy(early, c).wait_recv()
        release(c)

        @pl.when(has_outer)
        def _():
            edge(c)

        @pl.when(jnp.logical_not(has_outer))
        def _():
            relay_copy(c).start()

        sums = unit(own, 0, c)
        for e in range(count):
            acc[e, c] = sums[e]
        pl.when(has_outer)(lambda: edge_copy(c).start())
        return carry

    lax.fori_loop(0, parts, first_half, 0)

    def arrived(c):
        x_copy(late, c).wait_recv()
        release(parts + c)
        pl.when(has_outer)(lambda: relay_copy(c).start())

    def add(jobs):
        for (c, start, n), made in zip(jobs, [unit(far, 1, *job) for job in jobs]):
            for e in range(n):
                acc[start + e, c] += made[e]

    pl.when(has_outer)(lambda: arrived(0))

    def second_half(c, carry):
        pl.when(has_outer)(lambda: arrived(c + 1))
        pl.when(jnp.logical_not(has_outer))(lambda: arrived(c))
        relay_copy(c).wait_recv()
        add([(c, 0, count)])
        return carry

    lax.fori_loop(0, parts - 2, second_half, 0)
    last = parts - 1
    lower, upper, near = weights(last)
    for b in range(branches):
        for i, value in enumerate((lower[b], upper[b], jnp.where(near[b], 1.0, 0.0))):
            scales[i, pl.ds(b, 1)] = jnp.full((1, width), value, jnp.float32)
    c = last - 1

    @pl.when(has_outer)
    def _():
        arrived(last)
        relay_copy(c).wait_recv()
        add([(c, 0, count), (last, half * outer, half)])

    @pl.when(jnp.logical_not(has_outer))
    def _():
        arrived(c)
        relay_copy(c).wait_recv()
        add([(c, 0, count)])

    @pl.when(has_outer)
    def _():
        whole(edge_in, edge_recv)
        for c in range(parts):
            acc[(count - 1) * outer, c] += edge_in[c, 0].astype(jnp.float32)
            acc[1 + (count - 3) * outer, c] += edge_in[c, 1].astype(jnp.float32)

    pl.when(jnp.logical_not(has_outer))(lambda: arrived(last))
    relay_copy(last).wait_recv()
    whole(own, send.at[0])
    pl.when(has_outer)(lambda: whole(edge_out, send.at[1]))


def pair_finish(n_energy, sums, far, kbuf, kt, scales, out, held, sem):
    rank = lax.axis_index("energy")
    count, parts = sums.shape[:2]
    last, half = parts - 1, count // 2
    outer = rank % 2
    has_outer = jnp.where(outer == 0, rank, n_energy - 1 - rank) > 0

    def write(source, start, n, c):
        pltpu.make_async_copy(source, out.at[pl.ds(start, n), 0, c], sem).start()

    for c in range(last):
        write(sums.at[:, c], 0, count, c)

    def add(start, n):
        values = [far[start + e, last].astype(jnp.float32) for e in range(n + 2 * OFFMAX)]
        rows = [[scales[i, pl.ds(b, 1)] for b in range(kbuf.shape[1])] for i in range(3)]
        made = targets(values, kbuf.at[1], kt.at[1], rows[0], rows[1], [row > 0.5 for row in rows[2]])
        for e in range(n):
            held[e] = sums[start + e, last] + made[e]
            write(held.at[pl.ds(e, 1)], start + e, 1, last)

    @pl.when(has_outer)
    def _():
        write(sums.at[pl.ds(half * outer, half), last], half * outer, half, last)
        add(half * (1 - outer), half)

    pl.when(jnp.logical_not(has_outer))(lambda: add(0, count))
    pltpu.make_async_copy(sums, sums, sem).wait()


def pair_body(n_energy, green, offsets, occupation, coupling):
    count, slices, parts, width, _ = green.shape
    branches = coupling.shape[0]
    assert slices == 1 and count == 2 * OFFMAX
    assert 2 * branches % parts == 0 and 2 * branches <= 2 * OFFMAX * parts
    dma = pltpu.SemaphoreType.DMA
    regular = pltpu.SemaphoreType.REGULAR
    vmem = pl.BlockSpec(memory_space=pltpu.VMEM)
    made = pl.pallas_call(
        functools.partial(pair_kernel, n_energy),
        out_shape=[
            pltpu.VMEM((count, parts, width, width), jnp.float32),
            pltpu.VMEM((count + 2 * OFFMAX, parts, width, width), jnp.bfloat16),
            pltpu.VMEM((2, branches, width, width), jnp.bfloat16),
            pltpu.VMEM((2, branches * width, width), jnp.bfloat16),
            pltpu.VMEM((3, branches, width), jnp.float32),
        ],
        in_specs=[pl.BlockSpec(memory_space=pl.ANY)] * 4,
        out_specs=[vmem] * 5,
        scratch_shapes=[
            pltpu.SMEM(offsets.shape, offsets.dtype),
            pltpu.SMEM(occupation.shape, occupation.dtype),
            pltpu.VMEM((count + 2 * OFFMAX, parts, width, width), jnp.bfloat16),
            pltpu.VMEM((parts, OFFMAX, width, width), jnp.bfloat16),
            pltpu.VMEM((parts, OFFMAX, width, width), jnp.bfloat16),
            dma((3,)),
            regular,
            regular((2,)),
            dma((2,)),
            dma((2, parts)),
            dma,
            dma((parts,)),
            dma,
        ],
        compiler_params=pltpu.CompilerParams(collective_id=0, has_side_effects=True),
    )(offsets, occupation, green, coupling)
    return pl.pallas_call(
        functools.partial(pair_finish, n_energy),
        out_shape=jax.ShapeDtypeStruct(green.shape, jnp.float32),
        in_specs=[vmem] * 5,
        out_specs=pl.BlockSpec(memory_space=pl.ANY),
        scratch_shapes=[pltpu.VMEM((count, width, width), jnp.float32), dma],
    )(*[pltpu.with_memory_space_constraint(x, pltpu.VMEM) for x in made])


def solution(mesh):
    sizes = dict(mesh.shape)
    in_specs = (P("energy", "cuts", None, None, None), P(), P(), P(None, None, "cuts", None, None))
    out_specs = P("energy", "cuts", None, None, None)
    if sizes["cuts"] == 2 and sizes["energy"] % 2 == 0:
        step = functools.partial(pair_body, sizes["energy"])
    else:
        step = functools.partial(body, sizes["energy"], sizes["cuts"])
    return jax.shard_map(step, mesh=mesh, in_specs=in_specs, out_specs=out_specs, check_vma=False)
```

```python
import functools
import jax
import jax.numpy as jnp
from jax import lax
from jax.experimental import pallas as pl
from jax.experimental.pallas import tpu as pltpu
from jax.sharding import PartitionSpec as P

OFFMAX = 2
HOLD = ((3, 3, 4, 5), (2, 2, 3, 3))
MESH = pl.DeviceIdType.MESH


def kernel(n_energy, n_cuts, slots, offsets_in, occupation_in, green, coupling, acc,
           offsets, occupation, ext, kbuf, kt, small_sem, local_sem, k_sem,
           own_send, own_recv, x_send, x_recv, relay_send, relay_recv):
    rank = lax.axis_index("energy")
    cut = lax.axis_index("cuts")
    count, parts = ext.shape[2] - 2 * OFFMAX, ext.shape[1]
    branches, width = kbuf.shape[0], kbuf.shape[2]
    reach = OFFMAX
    first = rank % 2
    second = 1 - first

    def at(energy, slice_):
        return {"energy": energy, "cuts": slice_}

    has = (rank > 0, rank < n_energy - 1)
    beside = (jnp.maximum(rank - 1, 0), jnp.minimum(rank + 1, n_energy - 1))
    if slots == 1:
        partners = [(1, 1, 1 - cut, None, 2 - 2 * cut)]
    elif slots == 2:
        partners = [
            (1, 2, jnp.maximum(cut - 1, 0), cut > 0, 0),
            (2, 1, jnp.minimum(cut + 1, n_cuts - 1), cut < n_cuts - 1, 2),
        ]
    else:
        partners = []

    def when(cond, do):
        if cond is None:
            do()
        else:
            pl.when(cond)(do)

    def exists(p):
        return jnp.where(p == 0, rank, n_energy - 1 - rank) > 0

    def toward(p):
        return jnp.clip(rank + 2 * p - 1, 0, n_energy - 1)

    def source(p):
        return (count - reach) * p + reach

    def landing(p):
        return (count + reach) * (1 - p)

    def edge(p, c):
        return green.at[pl.ds((count - reach) * p, reach), 0, c]

    def own_copy(p, c):
        return pltpu.make_async_remote_copy(
            src_ref=edge(p, c),
            dst_ref=ext.at[0, c, pl.ds(landing(p), reach)],
            send_sem=own_send.at[p, c], recv_sem=own_recv.at[p, c],
            device_id=at(toward(p), cut), device_id_type=MESH)

    def relay_copy(slot, p, c):
        return pltpu.make_async_remote_copy(
            src_ref=ext.at[slot, c, pl.ds(source(p), reach)],
            dst_ref=ext.at[slot, c, pl.ds(landing(p), reach)],
            send_sem=relay_send.at[slot - 1, p, c], recv_sem=relay_recv.at[slot - 1, p, c],
            device_id=at(toward(p), cut), device_id_type=MESH)

    def x_copy(there, partner, p, c):
        return pltpu.make_async_remote_copy(
            src_ref=edge(p, c),
            dst_ref=ext.at[there, c, pl.ds(source(p), reach)],
            send_sem=x_send.at[there - 1, p, c], recv_sem=x_recv.at[there - 1, p, c],
            device_id=at(rank, partner), device_id_type=MESH)

    barrier = pltpu.get_barrier_semaphore()
    for p in range(2):
        pl.when(has[p])(functools.partial(
            pl.semaphore_signal, barrier, inc=1, device_id=at(beside[p], cut), device_id_type=MESH))
    for here, there, partner, cond, side in partners:
        when(cond, functools.partial(
            pl.semaphore_signal, barrier, inc=1, device_id=at(rank, partner), device_id_type=MESH))

    local = [pltpu.make_async_copy(green.at[:, 0, c], ext.at[0, c, pl.ds(reach, count)], local_sem.at[c])
             for c in range(parts)]
    for c in range(parts):
        local[c].start()
    k_copy = pltpu.make_async_copy(coupling.at[:, :, 0], kbuf, k_sem)
    k_copy.start()
    small = [pltpu.make_async_copy(offsets_in, offsets, small_sem.at[0]),
             pltpu.make_async_copy(occupation_in, occupation, small_sem.at[1])]
    for copy in small:
        copy.start()

    peers = sum(flag.astype(jnp.int32) for flag in has)
    for here, there, partner, cond, side in partners:
        peers = peers + (1 if cond is None else cond.astype(jnp.int32))
    pl.semaphore_wait(barrier, peers)

    order = [(0, 0)]
    for c in range(1, parts):
        order += [(0, c), (1, c - 1)]
    order += [(1, parts - 1)]
    for which, c in order:
        p = (first, second)[which]
        for here, there, partner, cond, side in partners:
            when(cond, lambda: x_copy(there, partner, p, c).start())
        if which == 0:
            for q in (first, second):
                pl.when(exists(q))(lambda: own_copy(q, c).start())

    @pl.when(rank == 0)
    def _():
        ext[:, :, pl.ds(0, reach)] = jnp.zeros((slots + 1, parts, reach, width, width), ext.dtype)

    @pl.when(rank == n_energy - 1)
    def _():
        ext[:, :, pl.ds(count + reach, reach)] = jnp.zeros((slots + 1, parts, reach, width, width), ext.dtype)

    k_copy.wait()
    for copy in small + local:
        copy.wait()
    for s in range(kbuf.shape[1]):
        for b in range(branches):
            kt[s, b * width:(b + 1) * width, :] = kbuf[b, s].T

    def forward(which, c):
        p = (first, second)[which]
        for here, there, partner, cond, side in partners:
            def go():
                x_copy(here, partner, p, c).wait_recv()
                pl.when(exists(p))(lambda: relay_copy(here, p, c).start())
            when(cond, go)

    def own_ready(c):
        for p in range(2):
            pl.when(has[p])(lambda: own_copy(1 - p, c).wait_recv())

    steps = parts * (slots + 1)
    last = 2 * parts - 2
    plan = {}
    for position, item in enumerate(order if partners else []):
        plan.setdefault(min(position, last), []).append(item)

    def compute(slot, side, c):
        values = [ext[slot, c, e].astype(jnp.float32) for e in range(count + 2 * reach)]
        lefts = []
        for b in range(branches):
            n = occupation[b]
            w = offsets[b]
            lesser = c < parts // 2
            lower = jnp.where(lesser, n, n + 1.0)
            upper = jnp.where(lesser, n + 1.0, n)
            low = [jnp.where(w == d, lower, 0.0) for d in range(1, reach + 1)]
            up = [jnp.where(w == d, upper, 0.0) for d in range(1, reach + 1)]
            mixed = []
            for e in range(count):
                total = None
                for d in range(1, reach + 1):
                    term = low[d - 1] * values[reach + e - d] + up[d - 1] * values[reach + e + d]
                    total = term if total is None else total + term
                mixed.append(total.astype(jnp.bfloat16))
            lefts.append(jnp.dot(kbuf[b, side], jnp.concatenate(mixed, axis=1),
                                 preferred_element_type=jnp.float32).astype(jnp.bfloat16))
        rows = [jnp.concatenate([left[:, e * width:(e + 1) * width] for left in lefts], axis=1)
                for e in range(count)]
        return jnp.dot(jnp.concatenate(rows, axis=0), kt[side], preferred_element_type=jnp.float32)

    def step(t, carry):
        slot = t // parts
        c = t % parts
        for k, todo in plan.items():
            @pl.when(t == k)
            def _():
                for which, part in todo:
                    forward(which, part)

        @pl.when(slot == 0)
        def _():
            own_ready(c)

        runs = slot == 0
        side = jnp.where(slot == 0, 1, 0)
        for here, there, partner, cond, which_side in partners:
            side = jnp.where(slot == here, which_side, side)
            mine = slot == here
            if cond is not None:
                mine = jnp.logical_and(mine, cond)
            runs = jnp.logical_or(runs, mine)

            @pl.when(mine)
            def _():
                for p in range(2):
                    pl.when(has[p])(lambda: relay_copy(here, 1 - p, c).wait_recv())

        def work():
            sums = compute(slot, side, c)

            @pl.when(slot == 0)
            def _():
                for e in range(count):
                    acc[c, e] = sums[e * width:(e + 1) * width]

            @pl.when(slot > 0)
            def _():
                for e in range(count):
                    acc[c, e] += sums[e * width:(e + 1) * width]

        if slots == 2:
            pl.when(runs)(work)
        else:
            work()

        return carry

    lax.fori_loop(0, steps, step, 0)

    for c in range(parts):
        for p in range(2):
            pl.when(has[p])(lambda: own_copy(p, c).wait_send())
            for here, there, partner, cond, side in partners:
                when(cond, lambda: x_copy(there, partner, p, c).wait_send())
                both = has[p] if cond is None else jnp.logical_and(cond, has[p])
                pl.when(both)(lambda: relay_copy(here, p, c).wait_send())


def write_out(sums, out, sem):
    copies = [pltpu.make_async_copy(sums.at[c], out.at[:, 0, c], sem.at[c]) for c in range(sums.shape[0])]
    for copy in copies:
        copy.start()
    for copy in copies:
        copy.wait()


def body(n_energy, n_cuts, green, offsets, occupation, coupling):
    count, slices, parts, width, _ = green.shape
    branches, sides = coupling.shape[:2]
    assert slices == 1 and count == 2 * OFFMAX
    slots = min(n_cuts - 1, 2)
    sems = max(slots, 1)
    dma = pltpu.SemaphoreType.DMA
    sums = pl.pallas_call(
        functools.partial(kernel, n_energy, n_cuts, slots),
        out_shape=pltpu.VMEM((parts, count, width, width), jnp.float32),
        in_specs=[
            pl.BlockSpec(memory_space=pl.ANY),
            pl.BlockSpec(memory_space=pl.ANY),
            pl.BlockSpec(memory_space=pl.ANY),
            pl.BlockSpec(memory_space=pl.ANY),
        ],
        out_specs=pl.BlockSpec(memory_space=pltpu.VMEM),
        scratch_shapes=[
            pltpu.SMEM(offsets.shape, offsets.dtype),
            pltpu.SMEM(occupation.shape, occupation.dtype),
            pltpu.VMEM((slots + 1, parts, count + 2 * OFFMAX, width, width), jnp.bfloat16),
            pltpu.VMEM((branches, sides, width, width), jnp.bfloat16),
            pltpu.VMEM((sides, branches * width, width), jnp.bfloat16),
            dma((2,)),
            dma((parts,)),
            dma,
            dma((2, parts)),
            dma((2, parts)),
            dma((sems, 2, parts)),
            dma((sems, 2, parts)),
            dma((sems, 2, parts)),
            dma((sems, 2, parts)),
        ],
        compiler_params=pltpu.CompilerParams(collective_id=0, has_side_effects=True),
    )(offsets, occupation, green, coupling)
    return pl.pallas_call(
        write_out,
        out_shape=jax.ShapeDtypeStruct(green.shape, jnp.float32),
        in_specs=[pl.BlockSpec(memory_space=pltpu.VMEM)],
        out_specs=pl.BlockSpec(memory_space=pl.ANY),
        scratch_shapes=[dma((parts,))],
    )(pltpu.with_memory_space_constraint(sums, pltpu.VMEM))


def targets(values, k, k_t, lower, upper, near):
    width, reach = k_t.shape[1], OFFMAX
    count = len(values) - 2 * reach
    lefts = []
    for b in range(k.shape[0]):
        mixed = []
        for e in range(reach, reach + count):
            below = jnp.where(near[b], values[e - 1], values[e - 2])
            above = jnp.where(near[b], values[e + 1], values[e + 2])
            mixed.append((lower[b] * below + upper[b] * above).astype(jnp.bfloat16))
        lefts.append(jnp.dot(k[b], jnp.concatenate(mixed, axis=1),
                             preferred_element_type=jnp.float32).astype(jnp.bfloat16))
    return [jnp.dot(jnp.concatenate([left[:, e * width:(e + 1) * width] for left in lefts], axis=1), k_t[...],
                    preferred_element_type=jnp.float32) for e in range(count)]


def pair_kernel(n_energy, offsets_in, occupation_in, green, coupling, acc, far, kbuf, kt, scales,
                offsets, occupation, own, edge_out, edge_in, local_sem,
                reply_x, reply_e, send, x_recv, own_recv, relay_recv, edge_recv):
    rank = lax.axis_index("energy")
    cut = lax.axis_index("cuts")
    reach = OFFMAX
    count, parts, width = own.shape[0] - 2 * reach, own.shape[1], own.shape[2]
    branches, half = kbuf.shape[1], count // 2
    outer = rank % 2
    inner = 1 - outer
    has_outer = jnp.where(outer == 0, rank, n_energy - 1 - rank) > 0
    early = jnp.where(has_outer, outer, inner)
    late = 1 - early
    core_peer = {"energy": rank + 1 - 2 * outer, "cuts": cut}
    chip_peer = {"energy": jnp.clip(rank - 1 + 2 * outer, 0, n_energy - 1), "cuts": cut}
    slice_peer = {"energy": rank, "cuts": 1 - cut}
    told = (rank + cut) % 2 == 0
    tells = (rank + cut) % 2 == 1

    def own_at(p):
        return pl.ds(reach + (count - reach) * p, reach)

    def halo_at(p):
        return pl.ds((count + reach) * p, reach)

    def edge_at(p):
        return pl.ds((count - reach) * p, reach)

    def x_copy(p, c):
        return pltpu.make_async_remote_copy(
            src_ref=green.at[edge_at(p), 0, c], dst_ref=far.at[own_at(p), c],
            send_sem=send.at[0], recv_sem=x_recv.at[p, c], device_id=slice_peer, device_id_type=MESH)

    def own_copy():
        return pltpu.make_async_remote_copy(
            src_ref=green.at[edge_at(inner), 0], dst_ref=own.at[halo_at(outer)],
            send_sem=send.at[0], recv_sem=own_recv, device_id=core_peer, device_id_type=MESH)

    def relay_copy(c):
        return pltpu.make_async_remote_copy(
            src_ref=far.at[own_at(inner), c], dst_ref=far.at[halo_at(outer), c],
            send_sem=send.at[0], recv_sem=relay_recv.at[c], device_id=core_peer, device_id_type=MESH)

    def edge_copy(c):
        return pltpu.make_async_remote_copy(
            src_ref=edge_out.at[c], dst_ref=edge_in.at[c],
            send_sem=send.at[1], recv_sem=edge_recv, device_id=chip_peer, device_id_type=MESH)

    def signal(sem, device):
        pl.semaphore_signal(sem, inc=1, device_id=device, device_id_type=MESH)

    barrier = pltpu.get_barrier_semaphore()

    @pl.when(tells)
    def _():
        signal(barrier, slice_peer)

    @pl.when(told)
    def _():
        signal(barrier, core_peer)

    @pl.when(jnp.logical_and(told, has_outer))
    def _():
        signal(barrier, chip_peer)

    @pl.when(told)
    def _():
        pl.semaphore_wait(barrier, 1)
        signal(reply_x, slice_peer)

    @pl.when(tells)
    def _():
        pl.semaphore_wait(reply_x, 1)

    held_back = jnp.logical_and(outer == 1, rank > 1)
    for c in range(parts):
        x_copy(early, c).start()

    @pl.when(jnp.logical_not(held_back))
    def _():
        for c in range(parts):
            x_copy(late, c).start()

    def release(point):
        for c in range(parts):
            at = jnp.where(cut == 0, HOLD[0][c], HOLD[1][c])
            pl.when(jnp.logical_and(held_back, point == at))(lambda: x_copy(late, c).start())

    loads = [pltpu.make_async_copy(green.at[:, 0], own.at[pl.ds(reach, count)], local_sem.at[0]),
             pltpu.make_async_copy(coupling.at[:, 1, 0], kbuf.at[0], local_sem.at[0]),
             pltpu.make_async_copy(coupling.at[:, 2 - 2 * cut, 0], kbuf.at[1], local_sem.at[0])]
    local = [pltpu.make_async_copy(offsets_in, offsets, local_sem.at[1]),
             pltpu.make_async_copy(occupation_in, occupation, local_sem.at[2])]
    for copy in loads + local:
        copy.start()

    def whole(ref, sem):
        pltpu.make_async_copy(ref, ref, sem).wait()

    @pl.when(tells)
    def _():
        pl.semaphore_wait(barrier, 1 + has_outer.astype(jnp.int32))
        signal(reply_e.at[0], core_peer)

    @pl.when(jnp.logical_and(tells, has_outer))
    def _():
        signal(reply_e.at[1], chip_peer)

    @pl.when(told)
    def _():
        pl.semaphore_wait(reply_e.at[0], 1)

    own_copy().start()

    own[halo_at(outer)] = jnp.zeros((reach, parts, width, width), own.dtype)
    far[halo_at(outer)] = jnp.zeros((reach, parts, width, width), far.dtype)
    whole(own.at[pl.ds(0, count + 2 * branches // parts)], local_sem.at[0])
    for copy in local:
        copy.wait()
    for s in range(2):
        for b in range(branches):
            kt[s, b * width:(b + 1) * width, :] = kbuf[s, b].T

    @pl.when(jnp.logical_and(told, has_outer))
    def _():
        pl.semaphore_wait(reply_e.at[1], 1)

    own_copy().wait_recv()

    def weights(c):
        lesser = c < parts // 2
        lower = [jnp.where(lesser, occupation[b], occupation[b] + 1.0) for b in range(branches)]
        upper = [jnp.where(lesser, occupation[b] + 1.0, occupation[b]) for b in range(branches)]
        return lower, upper, [offsets[b] == 1 for b in range(branches)]

    def unit(blocks, s, c, start=0, n=count):
        values = [blocks[start + e, c].astype(jnp.float32) for e in range(n + 2 * reach)]
        return targets(values, kbuf.at[s], kt.at[s], *weights(c))

    def edge(c):
        lower, upper, near = weights(c)
        lefts = []
        for s, blocks in enumerate((own, far)):
            first = blocks[reach + (count - 1) * outer, c].astype(jnp.float32)
            second = blocks[reach + 1 + (count - 3) * outer, c].astype(jnp.float32)
            for b in range(branches):
                gain = jnp.where(outer == 0, upper[b], lower[b])
                one = gain * jnp.where(near[b], first, second)
                two = jnp.where(near[b], 0.0, gain) * first
                both = jnp.concatenate([one.astype(jnp.bfloat16), two.astype(jnp.bfloat16)], axis=1)
                lefts.append(jnp.dot(kbuf[s, b], both, preferred_element_type=jnp.float32).astype(jnp.bfloat16))
        rows = [jnp.concatenate([left[:, e * width:(e + 1) * width] for left in lefts], axis=1)
                for e in range(reach)]
        sums = jnp.dot(jnp.concatenate(rows, axis=0), kt[...].reshape(2 * branches * width, width),
                       preferred_element_type=jnp.float32).astype(edge_out.dtype)
        for e in range(reach):
            edge_out[c, e] = sums[e * width:(e + 1) * width]

    def first_half(c, carry):
        x_copy(early, c).wait_recv()
        release(c)

        @pl.when(has_outer)
        def _():
            edge(c)

        @pl.when(jnp.logical_not(has_outer))
        def _():
            relay_copy(c).start()

        sums = unit(own, 0, c)
        for e in range(count):
            acc[e, c] = sums[e]
        pl.when(has_outer)(lambda: edge_copy(c).start())
        return carry

    lax.fori_loop(0, parts, first_half, 0)

    def arrived(c):
        x_copy(late, c).wait_recv()
        release(parts + c)
        pl.when(has_outer)(lambda: relay_copy(c).start())

    def add(jobs):
        for (c, start, n), made in zip(jobs, [unit(far, 1, *job) for job in jobs]):
            for e in range(n):
                acc[start + e, c] += made[e]

    pl.when(has_outer)(lambda: arrived(0))

    def second_half(c, carry):
        pl.when(has_outer)(lambda: arrived(c + 1))
        pl.when(jnp.logical_not(has_outer))(lambda: arrived(c))
        relay_copy(c).wait_recv()
        add([(c, 0, count)])
        return carry

    lax.fori_loop(0, parts - 2, second_half, 0)
    last = parts - 1
    lower, upper, near = weights(last)
    for b in range(branches):
        for i, value in enumerate((lower[b], upper[b], jnp.where(near[b], 1.0, 0.0))):
            scales[i, pl.ds(b, 1)] = jnp.full((1, width), value, jnp.float32)
    c = last - 1

    @pl.when(has_outer)
    def _():
        arrived(last)
        relay_copy(c).wait_recv()
        add([(c, 0, count), (last, half * outer, half)])

    @pl.when(jnp.logical_not(has_outer))
    def _():
        arrived(c)
        relay_copy(c).wait_recv()
        add([(c, 0, count)])

    @pl.when(has_outer)
    def _():
        whole(edge_in, edge_recv)
        for c in range(parts):
            acc[(count - 1) * outer, c] += edge_in[c, 0].astype(jnp.float32)
            acc[1 + (count - 3) * outer, c] += edge_in[c, 1].astype(jnp.float32)

    pl.when(jnp.logical_not(has_outer))(lambda: arrived(last))
    relay_copy(last).wait_recv()
    whole(own, send.at[0])
    pl.when(has_outer)(lambda: whole(edge_out, send.at[1]))


def pair_finish(n_energy, sums, far, kbuf, kt, scales, out, held, sem):
    rank = lax.axis_index("energy")
    count, parts = sums.shape[:2]
    last, half = parts - 1, count // 2
    outer = rank % 2
    has_outer = jnp.where(outer == 0, rank, n_energy - 1 - rank) > 0

    def write(source, start, n, c):
        pltpu.make_async_copy(source, out.at[pl.ds(start, n), 0, c], sem).start()

    write(sums.at[:, pl.ds(0, last)], 0, count, pl.ds(0, last))

    def add(start, n):
        values = [far[start + e, last].astype(jnp.float32) for e in range(n + 2 * OFFMAX)]
        rows = [[scales[i, pl.ds(b, 1)] for b in range(kbuf.shape[1])] for i in range(3)]
        made = targets(values, kbuf.at[1], kt.at[1], rows[0], rows[1], [row > 0.5 for row in rows[2]])
        for e in range(n):
            held[e] = sums[start + e, last] + made[e]
            write(held.at[pl.ds(e, 1)], start + e, 1, last)

    @pl.when(has_outer)
    def _():
        write(sums.at[pl.ds(half * outer, half), last], half * outer, half, last)
        add(half * (1 - outer), half)

    pl.when(jnp.logical_not(has_outer))(lambda: add(0, count))
    pltpu.make_async_copy(sums, sums, sem).wait()


def pair_body(n_energy, green, offsets, occupation, coupling):
    count, slices, parts, width, _ = green.shape
    branches = coupling.shape[0]
    assert slices == 1 and count == 2 * OFFMAX
    assert 2 * branches % parts == 0 and 2 * branches <= 2 * OFFMAX * parts
    dma = pltpu.SemaphoreType.DMA
    regular = pltpu.SemaphoreType.REGULAR
    vmem = pl.BlockSpec(memory_space=pltpu.VMEM)
    made = pl.pallas_call(
        functools.partial(pair_kernel, n_energy),
        out_shape=[
            pltpu.VMEM((count, parts, width, width), jnp.float32),
            pltpu.VMEM((count + 2 * OFFMAX, parts, width, width), jnp.bfloat16),
            pltpu.VMEM((2, branches, width, width), jnp.bfloat16),
            pltpu.VMEM((2, branches * width, width), jnp.bfloat16),
            pltpu.VMEM((3, branches, width), jnp.float32),
        ],
        in_specs=[pl.BlockSpec(memory_space=pl.ANY)] * 4,
        out_specs=[vmem] * 5,
        scratch_shapes=[
            pltpu.SMEM(offsets.shape, offsets.dtype),
            pltpu.SMEM(occupation.shape, occupation.dtype),
            pltpu.VMEM((count + 2 * OFFMAX, parts, width, width), jnp.bfloat16),
            pltpu.VMEM((parts, OFFMAX, width, width), jnp.bfloat16),
            pltpu.VMEM((parts, OFFMAX, width, width), jnp.bfloat16),
            dma((3,)),
            regular,
            regular((2,)),
            dma((2,)),
            dma((2, parts)),
            dma,
            dma((parts,)),
            dma,
        ],
        compiler_params=pltpu.CompilerParams(collective_id=0, has_side_effects=True),
    )(offsets, occupation, green, coupling)
    return pl.pallas_call(
        functools.partial(pair_finish, n_energy),
        out_shape=jax.ShapeDtypeStruct(green.shape, jnp.float32),
        in_specs=[vmem] * 5,
        out_specs=pl.BlockSpec(memory_space=pl.ANY),
        scratch_shapes=[pltpu.VMEM((count, width, width), jnp.float32), dma],
    )(*[pltpu.with_memory_space_constraint(x, pltpu.VMEM) for x in made])


def solution(mesh):
    sizes = dict(mesh.shape)
    in_specs = (P("energy", "cuts", None, None, None), P(), P(), P(None, None, "cuts", None, None))
    out_specs = P("energy", "cuts", None, None, None)
    if sizes["cuts"] == 2 and sizes["energy"] % 2 == 0:
        step = functools.partial(pair_body, sizes["energy"])
    else:
        step = functools.partial(body, sizes["energy"], sizes["cuts"])
    return jax.shard_map(step, mesh=mesh, in_specs=in_specs, out_specs=out_specs, check_vma=False)
```

```python
import functools
import jax
import jax.numpy as jnp
from jax import lax
from jax.experimental import pallas as pl
from jax.experimental.pallas import tpu as pltpu
from jax.sharding import PartitionSpec as P

OFFMAX = 2
HOLD = ((3, 3, 4, 5), (2, 3, 3, 3))
MESH = pl.DeviceIdType.MESH


def kernel(n_energy, n_cuts, slots, offsets_in, occupation_in, green, coupling, acc,
           offsets, occupation, ext, kbuf, kt, small_sem, local_sem, k_sem,
           own_send, own_recv, x_send, x_recv, relay_send, relay_recv):
    rank = lax.axis_index("energy")
    cut = lax.axis_index("cuts")
    count, parts = ext.shape[2] - 2 * OFFMAX, ext.shape[1]
    branches, width = kbuf.shape[0], kbuf.shape[2]
    reach = OFFMAX
    first = rank % 2
    second = 1 - first

    def at(energy, slice_):
        return {"energy": energy, "cuts": slice_}

    has = (rank > 0, rank < n_energy - 1)
    beside = (jnp.maximum(rank - 1, 0), jnp.minimum(rank + 1, n_energy - 1))
    if slots == 1:
        partners = [(1, 1, 1 - cut, None, 2 - 2 * cut)]
    elif slots == 2:
        partners = [
            (1, 2, jnp.maximum(cut - 1, 0), cut > 0, 0),
            (2, 1, jnp.minimum(cut + 1, n_cuts - 1), cut < n_cuts - 1, 2),
        ]
    else:
        partners = []

    def when(cond, do):
        if cond is None:
            do()
        else:
            pl.when(cond)(do)

    def exists(p):
        return jnp.where(p == 0, rank, n_energy - 1 - rank) > 0

    def toward(p):
        return jnp.clip(rank + 2 * p - 1, 0, n_energy - 1)

    def source(p):
        return (count - reach) * p + reach

    def landing(p):
        return (count + reach) * (1 - p)

    def edge(p, c):
        return green.at[pl.ds((count - reach) * p, reach), 0, c]

    def own_copy(p, c):
        return pltpu.make_async_remote_copy(
            src_ref=edge(p, c),
            dst_ref=ext.at[0, c, pl.ds(landing(p), reach)],
            send_sem=own_send.at[p, c], recv_sem=own_recv.at[p, c],
            device_id=at(toward(p), cut), device_id_type=MESH)

    def relay_copy(slot, p, c):
        return pltpu.make_async_remote_copy(
            src_ref=ext.at[slot, c, pl.ds(source(p), reach)],
            dst_ref=ext.at[slot, c, pl.ds(landing(p), reach)],
            send_sem=relay_send.at[slot - 1, p, c], recv_sem=relay_recv.at[slot - 1, p, c],
            device_id=at(toward(p), cut), device_id_type=MESH)

    def x_copy(there, partner, p, c):
        return pltpu.make_async_remote_copy(
            src_ref=edge(p, c),
            dst_ref=ext.at[there, c, pl.ds(source(p), reach)],
            send_sem=x_send.at[there - 1, p, c], recv_sem=x_recv.at[there - 1, p, c],
            device_id=at(rank, partner), device_id_type=MESH)

    barrier = pltpu.get_barrier_semaphore()
    for p in range(2):
        pl.when(has[p])(functools.partial(
            pl.semaphore_signal, barrier, inc=1, device_id=at(beside[p], cut), device_id_type=MESH))
    for here, there, partner, cond, side in partners:
        when(cond, functools.partial(
            pl.semaphore_signal, barrier, inc=1, device_id=at(rank, partner), device_id_type=MESH))

    local = [pltpu.make_async_copy(green.at[:, 0, c], ext.at[0, c, pl.ds(reach, count)], local_sem.at[c])
             for c in range(parts)]
    for c in range(parts):
        local[c].start()
    k_copy = pltpu.make_async_copy(coupling.at[:, :, 0], kbuf, k_sem)
    k_copy.start()
    small = [pltpu.make_async_copy(offsets_in, offsets, small_sem.at[0]),
             pltpu.make_async_copy(occupation_in, occupation, small_sem.at[1])]
    for copy in small:
        copy.start()

    peers = sum(flag.astype(jnp.int32) for flag in has)
    for here, there, partner, cond, side in partners:
        peers = peers + (1 if cond is None else cond.astype(jnp.int32))
    pl.semaphore_wait(barrier, peers)

    order = [(0, 0)]
    for c in range(1, parts):
        order += [(0, c), (1, c - 1)]
    order += [(1, parts - 1)]
    for which, c in order:
        p = (first, second)[which]
        for here, there, partner, cond, side in partners:
            when(cond, lambda: x_copy(there, partner, p, c).start())
        if which == 0:
            for q in (first, second):
                pl.when(exists(q))(lambda: own_copy(q, c).start())

    @pl.when(rank == 0)
    def _():
        ext[:, :, pl.ds(0, reach)] = jnp.zeros((slots + 1, parts, reach, width, width), ext.dtype)

    @pl.when(rank == n_energy - 1)
    def _():
        ext[:, :, pl.ds(count + reach, reach)] = jnp.zeros((slots + 1, parts, reach, width, width), ext.dtype)

    k_copy.wait()
    for copy in small + local:
        copy.wait()
    for s in range(kbuf.shape[1]):
        for b in range(branches):
            kt[s, b * width:(b + 1) * width, :] = kbuf[b, s].T

    def forward(which, c):
        p = (first, second)[which]
        for here, there, partner, cond, side in partners:
            def go():
                x_copy(here, partner, p, c).wait_recv()
                pl.when(exists(p))(lambda: relay_copy(here, p, c).start())
            when(cond, go)

    def own_ready(c):
        for p in range(2):
            pl.when(has[p])(lambda: own_copy(1 - p, c).wait_recv())

    steps = parts * (slots + 1)
    last = 2 * parts - 2
    plan = {}
    for position, item in enumerate(order if partners else []):
        plan.setdefault(min(position, last), []).append(item)

    def compute(slot, side, c):
        values = [ext[slot, c, e].astype(jnp.float32) for e in range(count + 2 * reach)]
        lefts = []
        for b in range(branches):
            n = occupation[b]
            w = offsets[b]
            lesser = c < parts // 2
            lower = jnp.where(lesser, n, n + 1.0)
            upper = jnp.where(lesser, n + 1.0, n)
            low = [jnp.where(w == d, lower, 0.0) for d in range(1, reach + 1)]
            up = [jnp.where(w == d, upper, 0.0) for d in range(1, reach + 1)]
            mixed = []
            for e in range(count):
                total = None
                for d in range(1, reach + 1):
                    term = low[d - 1] * values[reach + e - d] + up[d - 1] * values[reach + e + d]
                    total = term if total is None else total + term
                mixed.append(total.astype(jnp.bfloat16))
            lefts.append(jnp.dot(kbuf[b, side], jnp.concatenate(mixed, axis=1),
                                 preferred_element_type=jnp.float32).astype(jnp.bfloat16))
        rows = [jnp.concatenate([left[:, e * width:(e + 1) * width] for left in lefts], axis=1)
                for e in range(count)]
        return jnp.dot(jnp.concatenate(rows, axis=0), kt[side], preferred_element_type=jnp.float32)

    def step(t, carry):
        slot = t // parts
        c = t % parts
        for k, todo in plan.items():
            @pl.when(t == k)
            def _():
                for which, part in todo:
                    forward(which, part)

        @pl.when(slot == 0)
        def _():
            own_ready(c)

        runs = slot == 0
        side = jnp.where(slot == 0, 1, 0)
        for here, there, partner, cond, which_side in partners:
            side = jnp.where(slot == here, which_side, side)
            mine = slot == here
            if cond is not None:
                mine = jnp.logical_and(mine, cond)
            runs = jnp.logical_or(runs, mine)

            @pl.when(mine)
            def _():
                for p in range(2):
                    pl.when(has[p])(lambda: relay_copy(here, 1 - p, c).wait_recv())

        def work():
            sums = compute(slot, side, c)

            @pl.when(slot == 0)
            def _():
                for e in range(count):
                    acc[c, e] = sums[e * width:(e + 1) * width]

            @pl.when(slot > 0)
            def _():
                for e in range(count):
                    acc[c, e] += sums[e * width:(e + 1) * width]

        if slots == 2:
            pl.when(runs)(work)
        else:
            work()

        return carry

    lax.fori_loop(0, steps, step, 0)

    for c in range(parts):
        for p in range(2):
            pl.when(has[p])(lambda: own_copy(p, c).wait_send())
            for here, there, partner, cond, side in partners:
                when(cond, lambda: x_copy(there, partner, p, c).wait_send())
                both = has[p] if cond is None else jnp.logical_and(cond, has[p])
                pl.when(both)(lambda: relay_copy(here, p, c).wait_send())


def write_out(sums, out, sem):
    copies = [pltpu.make_async_copy(sums.at[c], out.at[:, 0, c], sem.at[c]) for c in range(sums.shape[0])]
    for copy in copies:
        copy.start()
    for copy in copies:
        copy.wait()


def body(n_energy, n_cuts, green, offsets, occupation, coupling):
    count, slices, parts, width, _ = green.shape
    branches, sides = coupling.shape[:2]
    assert slices == 1 and count == 2 * OFFMAX
    slots = min(n_cuts - 1, 2)
    sems = max(slots, 1)
    dma = pltpu.SemaphoreType.DMA
    sums = pl.pallas_call(
        functools.partial(kernel, n_energy, n_cuts, slots),
        out_shape=pltpu.VMEM((parts, count, width, width), jnp.float32),
        in_specs=[
            pl.BlockSpec(memory_space=pl.ANY),
            pl.BlockSpec(memory_space=pl.ANY),
            pl.BlockSpec(memory_space=pl.ANY),
            pl.BlockSpec(memory_space=pl.ANY),
        ],
        out_specs=pl.BlockSpec(memory_space=pltpu.VMEM),
        scratch_shapes=[
            pltpu.SMEM(offsets.shape, offsets.dtype),
            pltpu.SMEM(occupation.shape, occupation.dtype),
            pltpu.VMEM((slots + 1, parts, count + 2 * OFFMAX, width, width), jnp.bfloat16),
            pltpu.VMEM((branches, sides, width, width), jnp.bfloat16),
            pltpu.VMEM((sides, branches * width, width), jnp.bfloat16),
            dma((2,)),
            dma((parts,)),
            dma,
            dma((2, parts)),
            dma((2, parts)),
            dma((sems, 2, parts)),
            dma((sems, 2, parts)),
            dma((sems, 2, parts)),
            dma((sems, 2, parts)),
        ],
        compiler_params=pltpu.CompilerParams(collective_id=0, has_side_effects=True),
    )(offsets, occupation, green, coupling)
    return pl.pallas_call(
        write_out,
        out_shape=jax.ShapeDtypeStruct(green.shape, jnp.float32),
        in_specs=[pl.BlockSpec(memory_space=pltpu.VMEM)],
        out_specs=pl.BlockSpec(memory_space=pl.ANY),
        scratch_shapes=[dma((parts,))],
    )(pltpu.with_memory_space_constraint(sums, pltpu.VMEM))


def targets(values, k, k_t, lower, upper, near):
    width, reach = k_t.shape[1], OFFMAX
    count = len(values) - 2 * reach
    lefts = []
    for b in range(k.shape[0]):
        mixed = []
        for e in range(reach, reach + count):
            below = jnp.where(near[b], values[e - 1], values[e - 2])
            above = jnp.where(near[b], values[e + 1], values[e + 2])
            mixed.append((lower[b] * below + upper[b] * above).astype(jnp.bfloat16))
        lefts.append(jnp.dot(k[b], jnp.concatenate(mixed, axis=1),
                             preferred_element_type=jnp.float32).astype(jnp.bfloat16))
    return [jnp.dot(jnp.concatenate([left[:, e * width:(e + 1) * width] for left in lefts], axis=1), k_t[...],
                    preferred_element_type=jnp.float32) for e in range(count)]


def pair_kernel(n_energy, offsets_in, occupation_in, green, coupling, acc, far, kbuf, kt, scales,
                offsets, occupation, own, edge_out, edge_in, local_sem,
                reply_x, reply_e, send, x_recv, own_recv, relay_recv, edge_recv):
    rank = lax.axis_index("energy")
    cut = lax.axis_index("cuts")
    reach = OFFMAX
    count, parts, width = own.shape[0] - 2 * reach, own.shape[1], own.shape[2]
    branches, half = kbuf.shape[1], count // 2
    outer = rank % 2
    inner = 1 - outer
    has_outer = jnp.where(outer == 0, rank, n_energy - 1 - rank) > 0
    early = jnp.where(has_outer, outer, inner)
    late = 1 - early
    core_peer = {"energy": rank + 1 - 2 * outer, "cuts": cut}
    chip_peer = {"energy": jnp.clip(rank - 1 + 2 * outer, 0, n_energy - 1), "cuts": cut}
    slice_peer = {"energy": rank, "cuts": 1 - cut}
    told = (rank + cut) % 2 == 0
    tells = (rank + cut) % 2 == 1

    def own_at(p):
        return pl.ds(reach + (count - reach) * p, reach)

    def halo_at(p):
        return pl.ds((count + reach) * p, reach)

    def edge_at(p):
        return pl.ds((count - reach) * p, reach)

    def x_copy(p, c):
        return pltpu.make_async_remote_copy(
            src_ref=green.at[edge_at(p), 0, c], dst_ref=far.at[own_at(p), c],
            send_sem=send.at[0], recv_sem=x_recv.at[p, c], device_id=slice_peer, device_id_type=MESH)

    def own_copy():
        return pltpu.make_async_remote_copy(
            src_ref=green.at[edge_at(inner), 0], dst_ref=own.at[halo_at(outer)],
            send_sem=send.at[0], recv_sem=own_recv, device_id=core_peer, device_id_type=MESH)

    def relay_copy(c):
        return pltpu.make_async_remote_copy(
            src_ref=far.at[own_at(inner), c], dst_ref=far.at[halo_at(outer), c],
            send_sem=send.at[0], recv_sem=relay_recv.at[c], device_id=core_peer, device_id_type=MESH)

    def edge_copy(c):
        return pltpu.make_async_remote_copy(
            src_ref=edge_out.at[c], dst_ref=edge_in.at[c],
            send_sem=send.at[1], recv_sem=edge_recv, device_id=chip_peer, device_id_type=MESH)

    def signal(sem, device):
        pl.semaphore_signal(sem, inc=1, device_id=device, device_id_type=MESH)

    barrier = pltpu.get_barrier_semaphore()

    @pl.when(tells)
    def _():
        signal(barrier, slice_peer)

    @pl.when(told)
    def _():
        signal(barrier, core_peer)

    @pl.when(jnp.logical_and(told, has_outer))
    def _():
        signal(barrier, chip_peer)

    @pl.when(told)
    def _():
        pl.semaphore_wait(barrier, 1)
        signal(reply_x, slice_peer)

    @pl.when(tells)
    def _():
        pl.semaphore_wait(reply_x, 1)

    held_back = jnp.logical_and(outer == 1, rank > 1)
    for c in range(parts):
        x_copy(early, c).start()

    @pl.when(jnp.logical_not(held_back))
    def _():
        for c in range(parts):
            x_copy(late, c).start()

    def release(point):
        for c in range(parts):
            at = jnp.where(cut == 0, HOLD[0][c], HOLD[1][c])
            pl.when(jnp.logical_and(held_back, point == at))(lambda: x_copy(late, c).start())

    local = [pltpu.make_async_copy(green.at[:, 0], own.at[pl.ds(reach, count)], local_sem.at[0]),
             pltpu.make_async_copy(offsets_in, offsets, local_sem.at[1]),
             pltpu.make_async_copy(occupation_in, occupation, local_sem.at[2])]
    for copy in local:
        copy.start()
    pltpu.make_async_copy(coupling.at[:, 1, 0], kbuf.at[0], local_sem.at[3]).start()
    pltpu.make_async_copy(coupling.at[:, 2 - 2 * cut, 0], kbuf.at[1], local_sem.at[3]).start()

    def whole(ref, sem):
        pltpu.make_async_copy(ref, ref, sem).wait()

    @pl.when(tells)
    def _():
        pl.semaphore_wait(barrier, 1 + has_outer.astype(jnp.int32))
        signal(reply_e.at[0], core_peer)

    @pl.when(jnp.logical_and(tells, has_outer))
    def _():
        signal(reply_e.at[1], chip_peer)

    @pl.when(told)
    def _():
        pl.semaphore_wait(reply_e.at[0], 1)

    own_copy().start()

    own[halo_at(outer)] = jnp.zeros((reach, parts, width, width), own.dtype)
    far[halo_at(outer)] = jnp.zeros((reach, parts, width, width), far.dtype)
    whole(kbuf, local_sem.at[3])
    for copy in local:
        copy.wait()
    for s in range(2):
        for b in range(branches):
            kt[s, b * width:(b + 1) * width, :] = kbuf[s, b].T

    @pl.when(jnp.logical_and(told, has_outer))
    def _():
        pl.semaphore_wait(reply_e.at[1], 1)

    own_copy().wait_recv()

    def weights(c):
        lesser = c < parts // 2
        lower = [jnp.where(lesser, occupation[b], occupation[b] + 1.0) for b in range(branches)]
        upper = [jnp.where(lesser, occupation[b] + 1.0, occupation[b]) for b in range(branches)]
        return lower, upper, [offsets[b] == 1 for b in range(branches)]

    def unit(blocks, s, c, start=0, n=count):
        values = [blocks[start + e, c].astype(jnp.float32) for e in range(n + 2 * reach)]
        return targets(values, kbuf.at[s], kt.at[s], *weights(c))

    def edge(c):
        lower, upper, near = weights(c)
        lefts = []
        for s, blocks in enumerate((own, far)):
            first = blocks[reach + (count - 1) * outer, c].astype(jnp.float32)
            second = blocks[reach + 1 + (count - 3) * outer, c].astype(jnp.float32)
            for b in range(branches):
                gain = jnp.where(outer == 0, upper[b], lower[b])
                one = gain * jnp.where(near[b], first, second)
                two = jnp.where(near[b], 0.0, gain) * first
                both = jnp.concatenate([one.astype(jnp.bfloat16), two.astype(jnp.bfloat16)], axis=1)
                lefts.append(jnp.dot(kbuf[s, b], both, preferred_element_type=jnp.float32).astype(jnp.bfloat16))
        rows = [jnp.concatenate([left[:, e * width:(e + 1) * width] for left in lefts], axis=1)
                for e in range(reach)]
        sums = jnp.dot(jnp.concatenate(rows, axis=0), kt[...].reshape(2 * branches * width, width),
                       preferred_element_type=jnp.float32).astype(edge_out.dtype)
        for e in range(reach):
            edge_out[c, e] = sums[e * width:(e + 1) * width]

    def first_half(c, carry):
        x_copy(early, c).wait_recv()
        release(c)

        @pl.when(has_outer)
        def _():
            edge(c)

        @pl.when(jnp.logical_not(has_outer))
        def _():
            relay_copy(c).start()

        sums = unit(own, 0, c)
        for e in range(count):
            acc[e, c] = sums[e]
        pl.when(has_outer)(lambda: edge_copy(c).start())
        return carry

    lax.fori_loop(0, parts, first_half, 0)

    def arrived(c):
        x_copy(late, c).wait_recv()
        release(parts + c)
        pl.when(has_outer)(lambda: relay_copy(c).start())

    def add(jobs):
        for (c, start, n), made in zip(jobs, [unit(far, 1, *job) for job in jobs]):
            for e in range(n):
                acc[start + e, c] += made[e]

    pl.when(has_outer)(lambda: arrived(0))

    def second_half(c, carry):
        pl.when(has_outer)(lambda: arrived(c + 1))
        pl.when(jnp.logical_not(has_outer))(lambda: arrived(c))
        relay_copy(c).wait_recv()
        add([(c, 0, count)])
        return carry

    lax.fori_loop(0, parts - 2, second_half, 0)
    last = parts - 1
    lower, upper, near = weights(last)
    for b in range(branches):
        for i, value in enumerate((lower[b], upper[b], jnp.where(near[b], 1.0, 0.0))):
            scales[i, pl.ds(b, 1)] = jnp.full((1, width), value, jnp.float32)
    c = last - 1

    @pl.when(has_outer)
    def _():
        arrived(last)
        relay_copy(c).wait_recv()
        add([(c, 0, count), (last, half * outer, half)])

    @pl.when(jnp.logical_not(has_outer))
    def _():
        arrived(c)
        relay_copy(c).wait_recv()
        add([(c, 0, count)])

    @pl.when(has_outer)
    def _():
        whole(edge_in, edge_recv)
        for c in range(parts):
            acc[(count - 1) * outer, c] += edge_in[c, 0].astype(jnp.float32)
            acc[1 + (count - 3) * outer, c] += edge_in[c, 1].astype(jnp.float32)

    pl.when(jnp.logical_not(has_outer))(lambda: arrived(last))
    relay_copy(last).wait_recv()
    whole(own, send.at[0])
    pl.when(has_outer)(lambda: whole(edge_out, send.at[1]))


def pair_finish(n_energy, sums, far, kbuf, kt, scales, out, held, sem):
    rank = lax.axis_index("energy")
    count, parts = sums.shape[:2]
    last, half = parts - 1, count // 2
    outer = rank % 2
    has_outer = jnp.where(outer == 0, rank, n_energy - 1 - rank) > 0

    def write(source, start, n, c):
        pltpu.make_async_copy(source, out.at[pl.ds(start, n), 0, c], sem).start()

    for c in range(last):
        write(sums.at[:, c], 0, count, c)

    def add(start, n):
        values = [far[start + e, last].astype(jnp.float32) for e in range(n + 2 * OFFMAX)]
        rows = [[scales[i, pl.ds(b, 1)] for b in range(kbuf.shape[1])] for i in range(3)]
        made = targets(values, kbuf.at[1], kt.at[1], rows[0], rows[1], [row > 0.5 for row in rows[2]])
        for e in range(n):
            held[e] = sums[start + e, last] + made[e]
            write(held.at[pl.ds(e, 1)], start + e, 1, last)

    @pl.when(has_outer)
    def _():
        write(sums.at[pl.ds(half * outer, half), last], half * outer, half, last)
        add(half * (1 - outer), half)

    pl.when(jnp.logical_not(has_outer))(lambda: add(0, count))
    pltpu.make_async_copy(sums, sums, sem).wait()


def pair_body(n_energy, green, offsets, occupation, coupling):
    count, slices, parts, width, _ = green.shape
    branches = coupling.shape[0]
    assert slices == 1 and count == 2 * OFFMAX
    dma = pltpu.SemaphoreType.DMA
    regular = pltpu.SemaphoreType.REGULAR
    vmem = pl.BlockSpec(memory_space=pltpu.VMEM)
    made = pl.pallas_call(
        functools.partial(pair_kernel, n_energy),
        out_shape=[
            pltpu.VMEM((count, parts, width, width), jnp.float32),
            pltpu.VMEM((count + 2 * OFFMAX, parts, width, width), jnp.bfloat16),
            pltpu.VMEM((2, branches, width, width), jnp.bfloat16),
            pltpu.VMEM((2, branches * width, width), jnp.bfloat16),
            pltpu.VMEM((3, branches, width), jnp.float32),
        ],
        in_specs=[pl.BlockSpec(memory_space=pl.ANY)] * 4,
        out_specs=[vmem] * 5,
        scratch_shapes=[
            pltpu.SMEM(offsets.shape, offsets.dtype),
            pltpu.SMEM(occupation.shape, occupation.dtype),
            pltpu.VMEM((count + 2 * OFFMAX, parts, width, width), jnp.bfloat16),
            pltpu.VMEM((parts, OFFMAX, width, width), jnp.bfloat16),
            pltpu.VMEM((parts, OFFMAX, width, width), jnp.bfloat16),
            dma((4,)),
            regular,
            regular((2,)),
            dma((2,)),
            dma((2, parts)),
            dma,
            dma((parts,)),
            dma,
        ],
        compiler_params=pltpu.CompilerParams(collective_id=0, has_side_effects=True),
    )(offsets, occupation, green, coupling)
    return pl.pallas_call(
        functools.partial(pair_finish, n_energy),
        out_shape=jax.ShapeDtypeStruct(green.shape, jnp.float32),
        in_specs=[vmem] * 5,
        out_specs=pl.BlockSpec(memory_space=pl.ANY),
        scratch_shapes=[pltpu.VMEM((count, width, width), jnp.float32), dma],
    )(*[pltpu.with_memory_space_constraint(x, pltpu.VMEM) for x in made])


def solution(mesh):
    sizes = dict(mesh.shape)
    in_specs = (P("energy", "cuts", None, None, None), P(), P(), P(None, None, "cuts", None, None))
    out_specs = P("energy", "cuts", None, None, None)
    if sizes["cuts"] == 2 and sizes["energy"] % 2 == 0:
        step = functools.partial(pair_body, sizes["energy"])
    else:
        step = functools.partial(body, sizes["energy"], sizes["cuts"])
    return jax.shard_map(step, mesh=mesh, in_specs=in_specs, out_specs=out_specs, check_vma=False)
```
